32 devices in a mesh: gx: 4 (over y, x), gy: 4 (over z), gz: 2 (over core).
Axes of the slice: x: 2, y: 2, z: 4, core: 2. Of those that a mesh axis runs over, the one named last changes fastest.
Arguments:
- nodal_scalar_values: float32 [3, 32, 32, 4096], P(None, 'gx', 'gy', 'gz'), may hold values from -6 to 6
- geometry: float32 [6, 4, 4, 512], P(None, 'gx', 'gy', 'gz'), may hold values from -1.2 to 4, as said below
Outputs:
- assembled: float32 [3, 32, 32, 4096], P(None, 'gx', 'gy', 'gz')
The draws below stay inside these ranges and needn't reach their ends.
Inputs may be any that keep to these rules, and one draw needn't show every extreme that they name: `geometry`: G00, G11 and G22 are positive; each off-diagonal factor is at most 0.3 times the root of the product of its two diagonal factors in magnitude.
All inputs are finite; a program needn't handle non-finite values.
Results may differ from the reference program's by a relative error of at most 0.00007.
Values sent between devices are 32-bit elements; how exact they have to be, the bound alone decides.
A program may use at most 64 MiB of HBM per device.

```python
import math
import jax
import jax.numpy as jnp
import numpy as np
from jax import lax

COMPONENTS = 3
ELEMENTS_FIRST = 4
ELEMENTS_SECOND = 4
ELEMENTS_THIRD = 512


def draw_geometry(key, part):
    element_grid_shape = (ELEMENTS_FIRST, ELEMENTS_SECOND, ELEMENTS_THIRD)
    key_list = jax.random.split(key, 2)
    diagonal = jnp.exp(jax.random.uniform(key_list[0], (3,) + element_grid_shape, jnp.float32, math.log(0.5), math.log(2.0)))
    coupling = jax.random.uniform(key_list[1], (3,) + element_grid_shape, jnp.float32, -0.3, 0.3)
    cross_xy = coupling[0] * jnp.sqrt(diagonal[0] * diagonal[1])
    cross_xz = coupling[1] * jnp.sqrt(diagonal[0] * diagonal[2])
    cross_yz = coupling[2] * jnp.sqrt(diagonal[1] * diagonal[2])
    return jnp.stack([diagonal[0], diagonal[1], diagonal[2], cross_xy, cross_xz, cross_yz]).astype(jnp.float32)


def level_of(own_key, extent, cuts, low, high):
    factor_of, own = 1.0, jax.random.fold_in(own_key, 6)
    for axis_at, blocks in cuts:
        steps = jnp.exp(jax.random.uniform(jax.random.fold_in(own, axis_at), (blocks,), jnp.float32, low / len(cuts), high / len(cuts)))
        factor_of = factor_of * jnp.repeat(steps, extent[axis_at] // blocks).reshape([-1 if axis == axis_at else 1 for axis in range(len(extent))])
    return factor_of


def gaussian(key, shape, scale, most, pieces=(), held_as=jnp.bfloat16):
    level = level_of(key, shape, pieces, -0.22, 0.18) if pieces else 1.0
    entries = jax.random.normal(key, shape, jnp.float32) * scale * level
    return jnp.minimum(jnp.maximum(entries, -most), most).astype(held_as)


def setup_inputs(seed: int = 0) -> dict:
    key_of = jax.random.split(jax.random.key(seed), 3)
    return {
        "nodal_scalar_values": gaussian(key_of[0], (COMPONENTS, 8 * ELEMENTS_FIRST, 8 * ELEMENTS_SECOND, 8 * ELEMENTS_THIRD), 1.0, 6.0, ((1, 4), (2, 4), (3, 2)), jnp.float32),
        "geometry": draw_geometry(jax.random.fold_in(key_of[2], 71), 0),
    }


interior_points = [-0.8717401485096066, -0.5917001814331423, -0.2092992179024789, 0.2092992179024789, 0.5917001814331423, 0.8717401485096066]


def legendre_seven(point):
    previous = 1.0
    current = point
    for order in range(1, 7):
        following = ((2 * order + 1) * point * current - order * previous) / (order + 1)
        previous = current
        current = following
    return current


def gll_tables():
    degree = 7
    points = [-1.0] + interior_points + [1.0]
    values = [legendre_seven(point) for point in points]
    node_count = degree + 1
    weights = np.array([2.0 / (degree * (degree + 1) * value * value) for value in values])
    derivative = np.zeros((node_count, node_count))
    for row_index in range(node_count):
        for col_index in range(node_count):
            if row_index != col_index:
                derivative[row_index, col_index] = values[row_index] / (values[col_index] * (points[row_index] - points[col_index]))
    derivative[0, 0] = -degree * (degree + 1) / 4.0
    derivative[node_count - 1, node_count - 1] = degree * (degree + 1) / 4.0
    return derivative, weights


def apply_axis(field_in, matrix, direction):
    length = field_in.shape[direction]
    block_size = math.gcd(length, 128)
    big_table = jnp.kron(jnp.eye(block_size // 8, dtype=jnp.float32), matrix)
    dim_list = list(field_in.shape)
    folded_shape = dim_list[:direction] + [length // block_size, block_size] + dim_list[direction + 1:]
    folded_field = field_in.reshape(folded_shape)
    patterns = ["nbyz,ab->nayz", "xnbz,ab->xnaz", "xynb,ab->xyna"]
    result = jnp.einsum(patterns[direction], folded_field, big_table, precision=lax.Precision.HIGHEST)
    return result.reshape(field_in.shape)


def expand(field_component, target):
    elem_x, elem_y, elem_z = field_component.shape
    spread = jnp.broadcast_to(field_component[:, None, :, None, :, None], (elem_x, 8, elem_y, 8, elem_z, 8))
    return spread.reshape(target)


def stiffness(field_in, geometry):
    derivative, weights = gll_tables()
    matrix = jnp.asarray(derivative, jnp.float32)
    weight_row = jnp.asarray(weights, jnp.float32)
    size_x, size_y, size_z = field_in.shape
    weight_x = jnp.tile(weight_row, size_x // 8)
    weight_y = jnp.tile(weight_row, size_y // 8)
    weight_z = jnp.tile(weight_row, size_z // 8)
    node_weight = weight_x[:, None, None] * weight_y[None, :, None] * weight_z[None, None, :]
    grad_x = apply_axis(field_in, matrix, 0)
    grad_y = apply_axis(field_in, matrix, 1)
    grad_z = apply_axis(field_in, matrix, 2)
    factors = [expand(geometry[index], field_in.shape) for index in range(6)]
    flux_x = node_weight * (factors[0] * grad_x + factors[3] * grad_y + factors[4] * grad_z)
    flux_y = node_weight * (factors[3] * grad_x + factors[1] * grad_y + factors[5] * grad_z)
    flux_z = node_weight * (factors[4] * grad_x + factors[5] * grad_y + factors[2] * grad_z)
    transposed = matrix.T
    return apply_axis(flux_x, transposed, 0) + apply_axis(flux_y, transposed, 1) + apply_axis(flux_z, transposed, 2)


def combine(middle, below_plane, above_plane, direction):
    length = middle.shape[direction]
    from_above = jnp.concatenate([lax.slice_in_dim(middle, 1, length, axis=direction), above_plane], axis=direction)
    from_below = jnp.concatenate([below_plane, lax.slice_in_dim(middle, 0, length - 1, axis=direction)], axis=direction)
    position = lax.broadcasted_iota(jnp.int32, middle.shape, direction) % 8
    return middle + jnp.where(position == 7, from_above, 0.0) + jnp.where(position == 0, from_below, 0.0)


def single_component(field_values, geometry):
    total_x, total_y, total_z = field_values.shape
    zblock = math.gcd(total_z, 1024)
    block_count = total_z // zblock
    field_blocks = jnp.moveaxis(field_values.reshape(total_x, total_y, block_count, zblock), 2, 0)
    geometries = jnp.moveaxis(geometry.reshape(6, geometry.shape[1], geometry.shape[2], block_count, zblock // 8), 3, 0)
    local_terms = lax.map(lambda operands: stiffness(operands[0], operands[1]), (field_blocks, geometries))
    local_terms = jnp.moveaxis(local_terms, 0, 2).reshape(field_values.shape)
    summed = local_terms
    for direction in range(3):
        plane_extents = list(summed.shape)
        plane_extents[direction] = 1
        zero_plane = jnp.zeros(plane_extents, jnp.float32)
        summed = combine(summed, zero_plane, zero_plane, direction)
    return summed


def reference(nodal_scalar_values, geometry):
    return jnp.stack([single_component(nodal_scalar_values[component], geometry) for component in range(COMPONENTS)])
```

```python
import functools

import jax
import jax.numpy as jnp
import numpy as np
from jax import lax
from jax.experimental import pallas as pl
from jax.experimental.pallas import tpu as pltpu
from jax.sharding import PartitionSpec as P

interior_points = [
    -0.8717401485096066,
    -0.5917001814331423,
    -0.2092992179024789,
    0.2092992179024789,
    0.5917001814331423,
    0.8717401485096066,
]
MESH = pl.DeviceIdType.MESH
STEP = 256
LANES = 128
X_FIRST = True
LAG = 5
BEHIND = 1


def legendre_seven(point):
    previous = 1.0
    current = point
    for order in range(1, 7):
        following = ((2 * order + 1) * point * current - order * previous) / (order + 1)
        previous = current
        current = following
    return current


def gll_tables():
    degree = 7
    points = [-1.0] + interior_points + [1.0]
    values = [legendre_seven(point) for point in points]
    node_count = degree + 1
    weights = np.array([2.0 / (degree * (degree + 1) * value * value) for value in values])
    derivative = np.zeros((node_count, node_count))
    for row_index in range(node_count):
        for col_index in range(node_count):
            if row_index != col_index:
                derivative[row_index, col_index] = values[row_index] / (
                    values[col_index] * (points[row_index] - points[col_index])
                )
    derivative[0, 0] = -degree * (degree + 1) / 4.0
    derivative[node_count - 1, node_count - 1] = degree * (degree + 1) / 4.0
    return (derivative, weights)


def halves(table):
    table = np.asarray(table, np.float32)
    high = table.astype(jnp.bfloat16)
    low = (table - high.astype(np.float32)).astype(jnp.bfloat16)
    return high, low


def tables():
    derivative, weights = gll_tables()
    eye = np.eye(8)
    plane_weight = np.kron(weights, weights)
    forward_xy = np.concatenate([np.kron(derivative, eye), np.kron(eye, derivative)], axis=0)
    back_xy = np.concatenate([np.kron(derivative.T, eye), np.kron(eye, derivative.T)], axis=1)
    back_xy = back_xy * np.tile(plane_weight, 2)[None, :]
    forward_z = np.kron(np.eye(16), derivative.T)
    back_z = np.kron(np.eye(16), derivative)
    high, low = halves(forward_xy)
    forward_xy = np.concatenate([high, high, low, low], axis=1)
    high, low = halves(back_xy)
    back_xy = np.concatenate(
        [np.concatenate([high, high], axis=1), np.concatenate([low, low], axis=1)], axis=0
    )
    high, low = halves(forward_z)
    forward_z = np.tile(np.concatenate([high, low], axis=1), (2, 1))
    high, low = halves(back_z)
    back_z = np.tile(np.concatenate([high, low], axis=1), (2, 1))
    matrices = np.concatenate([forward_xy, back_xy, forward_z, back_z], axis=0)
    plane = np.repeat(plane_weight[:, None], LANES, axis=1)
    along = np.repeat(np.tile(weights, LANES // 8)[None, :], 8, axis=0)
    scales = np.concatenate([plane, along], axis=0).astype(np.float32)
    return matrices, scales


def seat(comp, m):
    if m in (0, 7):
        return 0, 2 * comp + (1 if m == 7 else 0)
    if comp:
        return comp, m - 1
    return (m - 1) // 2, 6 + (m - 1) % 2


def split(value):
    high = value.astype(jnp.bfloat16)
    low = (value - high.astype(jnp.float32)).astype(jnp.bfloat16)
    return high, low


def product(left, right):
    return jnp.dot(left, right, preferred_element_type=jnp.float32)


def along_lanes(pairs, table):
    rows, width = pairs[0][0].shape
    spans = [slice(start, start + LANES) for start in range(0, width, LANES)]
    stacked = [
        jnp.concatenate([high[:, span], low[:, span]], axis=1)
        for high, low in pairs
        for span in spans
    ]
    twice = product(jnp.concatenate(stacked, axis=0), table)
    once = twice[:, :LANES] + twice[:, LANES:]
    pieces = [once[at * rows : (at + 1) * rows] for at in range(len(stacked))]
    return [
        jnp.concatenate(pieces[at : at + len(spans)], axis=1)
        for at in range(0, len(pieces), len(spans))
    ]


def chunk_order(count):
    return [0] + ([count - 1] if count > 1 else []) + list(range(1, count - 1))


def chunk_sets(order):
    first, rest = order[:2], order[2:]
    tail = rest[max(len(rest) - 2, 0) :]
    rest = rest[: max(len(rest) - 2, 0)]
    pairs = [rest[at : at + 2] for at in range(0, len(rest), 2)]
    return [[c] for c in first] + pairs + [[c] for c in tail]


def kernel(
    sizes,
    chunk,
    u_hbm,
    geo_hbm,
    mat_hbm,
    scale_hbm,
    out,
    u,
    geo,
    mat,
    scale,
    metric,
    local,
    x_out,
    y_out,
    x_in,
    y_in,
    z_out,
    z_in,
    relay,
    in_sem,
    const_sem,
    x_send,
    y_send,
    z_send,
    r_send,
    edge_recv,
    bulk_recv,
    y_recv,
    z_recv,
    r_recv,
):
    comps, _, _, total = u.shape
    count = total // chunk
    order = chunk_order(count)
    sets = chunk_sets(order)
    set_of = {c: at for at, members in enumerate(sets) for c in members}
    names = ("gx", "gy", "gz")
    place = {name: lax.axis_index(name) for name in names}
    below = {name: place[name] > 0 for name in names}
    above = {name: place[name] < sizes[name] - 1 for name in names}

    const_copies = [
        pltpu.make_async_copy(mat_hbm, mat, const_sem.at[0]),
        pltpu.make_async_copy(scale_hbm, scale, const_sem.at[1]),
        pltpu.make_async_copy(geo_hbm, geo, const_sem.at[2]),
    ]
    for copy in const_copies:
        copy.start()
    in_copies = {}
    for c in order:
        span = pl.ds(c * chunk, chunk)
        in_copies[c] = pltpu.make_async_copy(
            u_hbm.at[:, :, :, span], u.at[:, :, :, span], in_sem.at[c]
        )
        in_copies[c].start()

    barrier = pltpu.get_barrier_semaphore()
    for name in names:
        for there, by in ((below[name], -1), (above[name], 1)):

            @pl.when(there)
            def _(name=name, by=by):
                pl.semaphore_signal(
                    barrier, inc=1, device_id={name: place[name] + by}, device_id_type=MESH
                )

    detour = sizes["gx"] == 4
    relayed = order[: count * 3 // 4] if detour else []
    opposite = lax.rem(place["gx"] + 2, 4)
    if detour:
        pl.semaphore_signal(barrier, inc=1, device_id={"gx": opposite}, device_id_type=MESH)

    for side in range(2):
        there = below if side == 0 else above

        @pl.when(jnp.logical_not(there["gx"]))
        def _(side=side):
            x_in[side] = jnp.zeros(x_in.shape[1:], jnp.float32)

        @pl.when(jnp.logical_not(there["gy"]))
        def _(side=side):
            y_in[side] = jnp.zeros(y_in.shape[1:], jnp.float32)

        @pl.when(jnp.logical_not(there["gz"]))
        def _(side=side):
            z_in[side] = jnp.zeros(z_in.shape[1:], jnp.float32)

    for copy in const_copies:
        copy.wait()

    rows = jnp.concatenate(
        [geo[k, 0] for k in range(6)] + [jnp.zeros((2, geo.shape[-1]), jnp.float32)], axis=0
    )
    lane = lax.broadcasted_iota(jnp.int32, (8, LANES), 1)
    for tile in range(total // LANES):
        first = tile * (LANES // 8)
        block = rows[:, first // LANES * LANES : first // LANES * LANES + LANES]
        spread = jnp.take_along_axis(block, lane // 8 + first % LANES, axis=1)
        metric[:, tile * LANES : (tile + 1) * LANES] = spread * scale[64:72, :]

    def span_of(c):
        return pl.ds(c * chunk, chunk)

    def beside(name, side):
        return {name: place[name] + (1 if side == 0 else -1)}

    def remote(source, target, send, recv, device):
        return pltpu.make_async_remote_copy(
            source, target, send, recv, device_id=device, device_id_type=MESH
        )

    def edge_copy(side, c):
        at = (side, 0, slice(None), span_of(c))
        return remote(
            x_out.at[at], x_in.at[at], x_send.at[side], edge_recv.at[c], beside("gx", side)
        )

    def bulk_copy(side, c):
        at = (side, slice(1, None), slice(None), span_of(c))
        return remote(
            x_out.at[at],
            x_in.at[at],
            x_send.at[side],
            bulk_recv.at[set_of[c]],
            beside("gx", side),
        )

    def y_edge_copy(side, c):
        at = (side, 0, slice(None), span_of(c))
        return remote(
            y_out.at[at], y_in.at[at], y_send.at[side], y_recv.at[set_of[c]], beside("gy", side)
        )

    def y_bulk_copy(side, c):
        at = (side, slice(1, None), slice(None), span_of(c))
        return remote(
            y_out.at[at], y_in.at[at], y_send.at[side], y_recv.at[set_of[c]], beside("gy", side)
        )

    def z_copy(side):
        return remote(
            z_out.at[side], z_in.at[side], z_send.at[side], z_recv.at[side], beside("gz", side)
        )

    def middle(side):
        return place["gx"] == 1 + side

    def by_way_of(side):
        return 3 * (1 - side) if X_FIRST else 3 * side

    def hop_copy(side, c):
        return remote(
            x_out.at[side, 1:, :, span_of(c)],
            relay.at[:, :, span_of(c)],
            x_send.at[side],
            r_recv.at[relayed.index(c)],
            {"gx": by_way_of(side)},
        )

    def onward_copy(side, c):
        return remote(
            relay.at[:, :, span_of(c)],
            x_in.at[side, 1:, :, span_of(c)],
            r_send.at[0],
            bulk_recv.at[set_of[c]],
            {"gx": 2 - side},
        )

    def target(name, side):
        return above[name] if side == 0 else below[name]

    def source(name, side):
        return below[name] if side == 0 else above[name]

    def when_do(condition, act):
        @pl.when(condition)
        def _():
            act()

    def landed(name, ref, recv):
        def wait(part):
            remote(part, part, recv, recv, beside(name, 0)).wait_recv()

        if sizes[name] == 2:
            wait(ref.at[0])
        elif sizes[name] > 2:
            both = jnp.logical_and(below[name], above[name])
            when_do(both, lambda: wait(ref))
            when_do(jnp.logical_not(both), lambda: wait(ref.at[0]))

    def forward(c):
        for side in range(2):

            @pl.when(place["gx"] == by_way_of(side))
            def _(side=side):
                hop_copy(side, c).wait_recv()
                onward_copy(side, c).start()

    def send_bulk(c):
        for side in range(2):
            if c in relayed:
                straight = jnp.logical_and(target("gx", side), jnp.logical_not(middle(side)))
                when_do(straight, lambda: bulk_copy(side, c).start())
                when_do(middle(side), lambda: hop_copy(side, c).start())
            else:
                when_do(target("gx", side), lambda: bulk_copy(side, c).start())

    def y_edges(c):
        lanes = slice(c * chunk, (c + 1) * chunk)
        landed("gx", x_in.at[:, 0, :, span_of(c)], edge_recv.at[c])
        low, high = x_in[0, 0, :, lanes], x_in[1, 0, :, lanes]
        row = lax.broadcasted_iota(jnp.int32, low.shape, 0)
        even, edge = row % 2 == 0, row < 2 * comps
        extra = jnp.where(even, pltpu.roll(low, 7, 0), high)
        y_out[0, 0, :, lanes] = y_out[0, 0, :, lanes] + jnp.where(edge, extra, 0.0)
        extra = jnp.where(even, low, pltpu.roll(high, 1, 0))
        y_out[1, 0, :, lanes] = y_out[1, 0, :, lanes] + jnp.where(edge, extra, 0.0)
        for side in range(2):
            when_do(target("gy", side), lambda: y_edge_copy(side, c).start())

    forward_xy, back_xy = mat[0:128, :], mat[128:256, :]
    forward_z, back_z = mat[256:512, :], mat[512:768, :]

    greeted = sum(side[name].astype(jnp.int32) for name in names for side in (below, above))
    greeted = greeted + (1 if detour else 0)
    waiting, edging = list(relayed), list(order)
    for at, c in enumerate(order):
        in_copies[c].wait()
        for start in range(c * chunk, (c + 1) * chunk, STEP):
            lanes = slice(start, start + STEP)
            g00, g11, g22, g01, g02, g12 = [metric[k : k + 1, lanes] for k in range(6)]
            pairs = [split(u[comp, :, :, lanes].reshape(64, STEP)) for comp in range(comps)]
            planes = [
                product(forward_xy, jnp.concatenate([high, low, high, low], axis=0))
                for high, low in pairs
            ]
            grads_z = along_lanes(pairs, forward_z)
            sums, z_pairs = [], []
            for both, grad_z in zip(planes, grads_z):
                grad_x, grad_y = both[:64], both[64:]
                flux_x = g00 * grad_x + g01 * grad_y + g02 * grad_z
                flux_y = g01 * grad_x + g11 * grad_y + g12 * grad_z
                x_high, x_low = split(flux_x)
                y_high, y_low = split(flux_y)
                z_pairs.append(split(g02 * grad_x + g12 * grad_y + g22 * grad_z))
                sums.append(
                    product(back_xy, jnp.concatenate([x_high, y_high, x_low, y_low], axis=0))
                )
            backs_z = along_lanes(z_pairs, back_z)
            weight = jnp.concatenate([scale[0:64, :]] * (STEP // LANES), axis=1)
            for comp in range(comps):
                twice = sums[comp]
                terms = twice[:64] + twice[64:] + weight * backs_z[comp]
                terms = terms.reshape(8, 8, STEP)
                local[comp, :, :, lanes] = terms
                for n in range(8):
                    tile, row = seat(comp, n)
                    y_out[0, tile, row : row + 1, lanes] = terms[n, 7:8]
                    y_out[1, tile, row : row + 1, lanes] = terms[n, 0:1]
                    x_out[0, tile, row : row + 1, lanes] = terms[7, n : n + 1]
                    x_out[1, tile, row : row + 1, lanes] = terms[0, n : n + 1]
        if at == 0:
            pl.semaphore_wait(barrier, greeted)
        for side in range(2):
            when_do(target("gx", side), lambda: edge_copy(side, c).start())
            when_do(target("gy", side), lambda: y_bulk_copy(side, c).start())
        if at >= BEHIND:
            send_bulk(order[at - BEHIND])
        if at >= LAG and edging:
            y_edges(edging.pop(0))
        if at >= LAG + 1 and waiting:
            forward(waiting.pop(0))
    for c in order[count - min(BEHIND, count) :]:
        send_bulk(c)
    while waiting or edging:
        if edging:
            y_edges(edging.pop(0))
        if waiting:
            forward(waiting.pop(0))

    def xy_sum(comp, n, lanes):
        value = local[comp, n, :, lanes]
        tile, row = seat(comp, n)
        from_below = y_in[0, tile, row : row + 1, lanes]
        from_above = y_in[1, tile, row : row + 1, lanes]
        if n in (0, 7):
            x_side = 0 if n == 0 else 1
            seats = [seat(comp, m) for m in range(8)]
            rows = [x_in[x_side, tile, row : row + 1, lanes] for tile, row in seats]
            value = value + jnp.concatenate(rows, axis=0)
        where = lax.broadcasted_iota(jnp.int32, value.shape, 0)
        value = value + jnp.where(where == 0, from_below, 0.0)
        return value + jnp.where(where == 7, from_above, 0.0)

    def arrived(at):
        members = sets[at]
        span = pl.ds(members[0] * chunk, len(members) * chunk)
        landed("gx", x_in.at[:, 1:, :, span], bulk_recv.at[at])
        landed("gy", y_in.at[:, :, :, span], y_recv.at[at])

    def finish(first, last):
        for comp in range(comps):
            for n in range(8):
                value = xy_sum(comp, n, slice(max(first - LANES, 0), min(last + LANES, total)))
                if first == 0:
                    value = jnp.concatenate([z_in[0, comp, n], value], axis=1)
                if last == total:
                    value = jnp.concatenate([value, z_in[1, comp, n]], axis=1)
                width = value.shape[1]
                before = pltpu.roll(value, 1, 1)[:, LANES:-LANES]
                after = pltpu.roll(value, width - 1, 1)[:, LANES:-LANES]
                position = lax.broadcasted_iota(jnp.int32, before.shape, 1) % 8
                extra = jnp.where(position == 7, after, jnp.where(position == 0, before, 0.0))
                out[comp, n, :, first:last] = value[:, LANES:-LANES] + extra

    def sent(out_ref, in_ref, send, side):
        remote(out_ref.at[side], in_ref.at[side], send.at[side], send.at[side], beside("gz", 0)).wait_send()

    def onward_sent():
        part = relay.at[:, :, pl.ds(0, len(relayed) * chunk)]
        remote(part, part, r_send.at[0], r_send.at[0], beside("gz", 0)).wait_send()

    tiles = total // LANES
    todo, here = set(range(tiles)), set()
    ends_here = False
    for at, members in enumerate(sets):
        arrived(at)
        for c in members:
            here |= set(range(c * chunk // LANES, (c + 1) * chunk // LANES))
        if {0, tiles - 1} <= here and not ends_here:
            ends_here = True
            for side in range(2):
                lanes = slice(total - LANES, total) if side == 0 else slice(0, LANES)
                for comp in range(comps):
                    for n in range(8):
                        z_out[side, comp, n] = xy_sum(comp, n, lanes)
                when_do(target("gz", side), lambda: z_copy(side).start())
            if count > 2:
                continue
        if not ends_here:
            continue
        if {0, tiles - 1} <= todo:
            for side in range(2):
                when_do(source("gz", side), lambda: z_copy(side).wait_recv())
        ready = sorted(
            t for t in todo if all(0 > o or o >= tiles or o in here for o in (t - 1, t, t + 1))
        )
        todo -= set(ready)
        while ready:
            first = last = ready.pop(0)
            while ready and ready[0] == last + 1:
                last = ready.pop(0)
            finish(first * LANES, (last + 1) * LANES)

    for side in range(2):
        when_do(target("gx", side), lambda: sent(x_out, x_in, x_send, side))
        when_do(target("gy", side), lambda: sent(y_out, y_in, y_send, side))
        when_do(target("gz", side), lambda: z_copy(side).wait_send())
    if relayed:
        when_do(jnp.logical_or(place["gx"] == 0, place["gx"] == 3), onward_sent)


def local_part(sizes, nodal_scalar_values, geometry):
    comps, _, _, total = nodal_scalar_values.shape
    chunk = min(256, total)
    count = total // chunk
    sets = len(chunk_sets(chunk_order(count)))
    matrices, scales = tables()
    f32 = jnp.float32
    dma = pltpu.SemaphoreType.DMA
    any_space = pl.BlockSpec(memory_space=pl.ANY)
    plane = pltpu.VMEM((2, comps, 8, total), f32)
    column = pltpu.VMEM((2, comps, 8, 8, LANES), f32)
    return pl.pallas_call(
        functools.partial(kernel, sizes, chunk),
        out_shape=pltpu.VMEM(nodal_scalar_values.shape, f32),
        in_specs=[any_space] * 4,
        out_specs=pl.BlockSpec(memory_space=pltpu.VMEM),
        scratch_shapes=[
            pltpu.VMEM(nodal_scalar_values.shape, f32),
            pltpu.VMEM(geometry.shape, f32),
            pltpu.VMEM(matrices.shape, jnp.bfloat16),
            pltpu.VMEM(scales.shape, f32),
            pltpu.VMEM((8, total), f32),
            pltpu.VMEM(nodal_scalar_values.shape, f32),
            plane,
            plane,
            plane,
            plane,
            column,
            column,
            pltpu.VMEM((comps - 1, 8, total), f32),
            dma((count,)),
            dma((3,)),
            dma((2,)),
            dma((2,)),
            dma((2,)),
            dma((1,)),
            dma((count,)),
            dma((sets,)),
            dma((sets,)),
            dma((2,)),
            dma((max(count * 3 // 4, 1),)),
        ],
        compiler_params=pltpu.CompilerParams(collective_id=0, has_side_effects=True),
        name="poisson",
    )(nodal_scalar_values, geometry, jnp.asarray(matrices), jnp.asarray(scales))


def solution(mesh):
    return jax.shard_map(
        functools.partial(local_part, dict(mesh.shape)),
        mesh=mesh,
        in_specs=(P(None, "gx", "gy", "gz"), P(None, "gx", "gy", "gz")),
        out_specs=P(None, "gx", "gy", "gz"),
        check_vma=False,
    )
```

```python
import functools

import jax
import jax.numpy as jnp
import numpy as np
from jax import lax
from jax.experimental import pallas as pl
from jax.experimental.pallas import tpu as pltpu
from jax.sharding import PartitionSpec as P

interior_points = [
    -0.8717401485096066,
    -0.5917001814331423,
    -0.2092992179024789,
    0.2092992179024789,
    0.5917001814331423,
    0.8717401485096066,
]
MESH = pl.DeviceIdType.MESH
STEP = 512
LANES = 128
X_FIRST = True
LAG = 4
BEHIND = 2
X_EDGE = 7
Y_EDGE = (6, 7)


def legendre_seven(point):
    previous = 1.0
    current = point
    for order in range(1, 7):
        following = ((2 * order + 1) * point * current - order * previous) / (order + 1)
        previous = current
        current = following
    return current


def gll_tables():
    degree = 7
    points = [-1.0] + interior_points + [1.0]
    values = [legendre_seven(point) for point in points]
    node_count = degree + 1
    weights = np.array([2.0 / (degree * (degree + 1) * value * value) for value in values])
    derivative = np.zeros((node_count, node_count))
    for row_index in range(node_count):
        for col_index in range(node_count):
            if row_index != col_index:
                derivative[row_index, col_index] = values[row_index] / (
                    values[col_index] * (points[row_index] - points[col_index])
                )
    derivative[0, 0] = -degree * (degree + 1) / 4.0
    derivative[node_count - 1, node_count - 1] = degree * (degree + 1) / 4.0
    return (derivative, weights)


def halves(table):
    table = np.asarray(table, np.float32)
    high = table.astype(jnp.bfloat16)
    low = (table - high.astype(np.float32)).astype(jnp.bfloat16)
    return high, low


def tables():
    derivative, weights = gll_tables()
    eye = np.eye(8)
    plane_weight = np.kron(weights, weights)
    forward_xy = np.concatenate([np.kron(derivative, eye), np.kron(eye, derivative)], axis=0)
    back_xy = np.concatenate([np.kron(derivative.T, eye), np.kron(eye, derivative.T)], axis=1)
    back_xy = back_xy * np.tile(plane_weight, 2)[None, :]
    forward_z = np.kron(np.eye(16), derivative.T)
    back_z = np.kron(np.eye(16), derivative)
    high, low = halves(forward_xy)
    forward_xy = np.concatenate([high, high, low, low], axis=1)
    high, low = halves(back_xy)
    back_xy = np.concatenate(
        [np.concatenate([high, high], axis=1), np.concatenate([low, low], axis=1)], axis=0
    )
    high, low = halves(forward_z)
    forward_z = np.tile(np.concatenate([high, low], axis=1), (2, 1))
    high, low = halves(back_z)
    back_z = np.tile(np.concatenate([high, low], axis=1), (2, 1))
    matrices = np.concatenate([forward_xy, back_xy, forward_z, back_z], axis=0)
    plane = np.repeat(plane_weight[:, None], LANES, axis=1)
    along = np.repeat(np.tile(weights, LANES // 8)[None, :], 8, axis=0)
    scales = np.concatenate([plane, along], axis=0).astype(np.float32)
    return matrices, scales


def row_index(shape):
    return lax.broadcasted_iota(jnp.int32, shape, 0)


def pack(planes, edge):
    first, second, third = planes
    turn = (row_index(first.shape) + (8 - edge)) % 8
    own = turn < 2
    second_edge = jnp.logical_and(turn >= 2, turn < 4)
    third_edge = jnp.logical_and(turn >= 4, turn < 6)
    edges = jnp.where(
        second_edge,
        pltpu.roll(second, 2, 0),
        jnp.where(third_edge, pltpu.roll(third, 4, 0), first),
    )
    return [
        edges,
        jnp.where(own, pltpu.roll(first, 6, 0), second),
        jnp.where(own, pltpu.roll(first, 4, 0), third),
    ]


def unpack(tiles, comp, edge):
    turn = (row_index(tiles[0].shape) + (8 - edge)) % 8
    if comp:
        return jnp.where(turn < 2, pltpu.roll(tiles[0], 8 - 2 * comp, 0), tiles[comp])
    from_second = jnp.logical_and(turn >= 2, turn < 4)
    from_third = jnp.logical_and(turn >= 4, turn < 6)
    return jnp.where(
        from_second,
        pltpu.roll(tiles[1], 2, 0),
        jnp.where(from_third, pltpu.roll(tiles[2], 4, 0), tiles[0]),
    )


def y_planes(terms):
    turn = (row_index(terms[0].shape) + 1) % 8

    def gather(four):
        return jnp.where(
            turn < 2,
            four[0],
            jnp.where(
                turn < 4,
                pltpu.roll(four[1], 2, 0),
                jnp.where(turn < 6, pltpu.roll(four[2], 4, 0), pltpu.roll(four[3], 6, 0)),
            ),
        )

    low, high = gather(terms[:4]), pltpu.roll(gather(terms[4:]), 1, 0)
    even = turn % 2 == 0
    return jnp.where(even, low, high), jnp.where(even, high, low)


def y_seat(side, comp, n):
    edge = Y_EDGE[side]
    row = (2 * n + 7 + side) % 8 if n < 4 else 2 * (n - 4) + side
    turn = (row - edge) % 8
    if turn < 2:
        return 0, (row + 2 * comp) % 8
    if comp:
        return comp, row
    if turn < 6:
        return turn // 2, (row - 2 * (turn // 2)) % 8
    return 0, row


def split(value):
    high = value.astype(jnp.bfloat16)
    low = (value - high.astype(jnp.float32)).astype(jnp.bfloat16)
    return high, low


def product(left, right):
    return jnp.dot(left, right, preferred_element_type=jnp.float32)


def along_lanes(pairs, table):
    rows, width = pairs[0][0].shape
    spans = [slice(start, start + LANES) for start in range(0, width, LANES)]
    stacked = [
        jnp.concatenate([high[:, span], low[:, span]], axis=1)
        for high, low in pairs
        for span in spans
    ]
    twice = product(jnp.concatenate(stacked, axis=0), table)
    once = twice[:, :LANES] + twice[:, LANES:]
    pieces = [once[at * rows : (at + 1) * rows] for at in range(len(stacked))]
    return [
        jnp.concatenate(pieces[at : at + len(spans)], axis=1)
        for at in range(0, len(pieces), len(spans))
    ]


def chunk_order(count):
    return [0] + ([count - 1] if count > 1 else []) + list(range(1, count - 1))


def chunk_sets(order):
    first, rest = order[:2], order[2:]
    tail = rest[max(len(rest) - 2, 0) :]
    rest = rest[: max(len(rest) - 2, 0)]
    pairs = [rest[at : at + 2] for at in range(0, len(rest), 2)]
    return [[c] for c in first] + pairs + [[c] for c in tail]


def kernel(
    sizes,
    chunk,
    u_hbm,
    geo_hbm,
    mat_hbm,
    scale_hbm,
    out,
    u,
    geo,
    mat,
    scale,
    metric,
    local,
    x_out,
    y_out,
    x_in,
    y_in,
    z_out,
    z_in,
    relay,
    in_sem,
    const_sem,
    x_send,
    y_send,
    z_send,
    r_send,
    edge_recv,
    bulk_recv,
    y_recv,
    z_recv,
    r_recv,
):
    comps, _, _, total = u.shape
    count = total // chunk
    order = chunk_order(count)
    sets = chunk_sets(order)
    set_of = {c: at for at, members in enumerate(sets) for c in members}
    names = ("gx", "gy", "gz")
    place = {name: lax.axis_index(name) for name in names}
    below = {name: place[name] > 0 for name in names}
    above = {name: place[name] < sizes[name] - 1 for name in names}

    const_copies = [
        pltpu.make_async_copy(mat_hbm, mat, const_sem.at[0]),
        pltpu.make_async_copy(scale_hbm, scale, const_sem.at[1]),
        pltpu.make_async_copy(geo_hbm, geo, const_sem.at[2]),
    ]
    for copy in const_copies:
        copy.start()
    in_copies = {}
    for c in order:
        span = pl.ds(c * chunk, chunk)
        in_copies[c] = pltpu.make_async_copy(
            u_hbm.at[:, :, :, span], u.at[:, :, :, span], in_sem.at[c]
        )
        in_copies[c].start()

    barrier = pltpu.get_barrier_semaphore()
    for name in names:
        for there, by in ((below[name], -1), (above[name], 1)):

            @pl.when(there)
            def _(name=name, by=by):
                pl.semaphore_signal(
                    barrier, inc=1, device_id={name: place[name] + by}, device_id_type=MESH
                )

    detour = sizes["gx"] == 4
    relayed = order[: count * 3 // 4] if detour else []
    opposite = lax.rem(place["gx"] + 2, 4)
    if detour:
        pl.semaphore_signal(barrier, inc=1, device_id={"gx": opposite}, device_id_type=MESH)

    for side in range(2):
        there = below if side == 0 else above

        @pl.when(jnp.logical_not(there["gx"]))
        def _(side=side):
            x_in[side] = jnp.zeros(x_in.shape[1:], jnp.float32)

        @pl.when(jnp.logical_not(there["gy"]))
        def _(side=side):
            y_in[side] = jnp.zeros(y_in.shape[1:], jnp.float32)

        @pl.when(jnp.logical_not(there["gz"]))
        def _(side=side):
            z_in[side] = jnp.zeros(z_in.shape[1:], jnp.float32)

    for copy in const_copies:
        copy.wait()

    rows = jnp.concatenate(
        [geo[k, 0] for k in range(6)] + [jnp.zeros((2, geo.shape[-1]), jnp.float32)], axis=0
    )
    lane = lax.broadcasted_iota(jnp.int32, (8, LANES), 1)
    for tile in range(total // LANES):
        first = tile * (LANES // 8)
        block = rows[:, first // LANES * LANES : first // LANES * LANES + LANES]
        spread = jnp.take_along_axis(block, lane // 8 + first % LANES, axis=1)
        metric[:, tile * LANES : (tile + 1) * LANES] = spread * scale[64:72, :]

    def span_of(c):
        return pl.ds(c * chunk, chunk)

    def beside(name, side):
        return {name: place[name] + (1 if side == 0 else -1)}

    def remote(source, target, send, recv, device):
        return pltpu.make_async_remote_copy(
            source, target, send, recv, device_id=device, device_id_type=MESH
        )

    def edge_copy(side, c):
        at = (side, 0, slice(None), span_of(c))
        return remote(
            x_out.at[at], x_in.at[at], x_send.at[side], edge_recv.at[c], beside("gx", side)
        )

    def bulk_copy(side, c):
        at = (side, slice(1, None), slice(None), span_of(c))
        return remote(
            x_out.at[at],
            x_in.at[at],
            x_send.at[side],
            bulk_recv.at[set_of[c]],
            beside("gx", side),
        )

    def y_edge_copy(side, c):
        at = (side, 0, slice(None), span_of(c))
        return remote(
            y_out.at[at], y_in.at[at], y_send.at[side], y_recv.at[set_of[c]], beside("gy", side)
        )

    def y_bulk_copy(side, c):
        at = (side, slice(1, None), slice(None), span_of(c))
        return remote(
            y_out.at[at], y_in.at[at], y_send.at[side], y_recv.at[set_of[c]], beside("gy", side)
        )

    def z_copy(side):
        return remote(
            z_out.at[side], z_in.at[side], z_send.at[side], z_recv.at[side], beside("gz", side)
        )

    def middle(side):
        return place["gx"] == 1 + side

    def by_way_of(side):
        return 3 * (1 - side) if X_FIRST else 3 * side

    def hop_copy(side, c):
        return remote(
            x_out.at[side, 1:, :, span_of(c)],
            relay.at[:, :, span_of(c)],
            x_send.at[side],
            r_recv.at[relayed.index(c)],
            {"gx": by_way_of(side)},
        )

    def onward_copy(side, c):
        return remote(
            relay.at[:, :, span_of(c)],
            x_in.at[side, 1:, :, span_of(c)],
            r_send.at[0],
            bulk_recv.at[set_of[c]],
            {"gx": 2 - side},
        )

    def target(name, side):
        return above[name] if side == 0 else below[name]

    def source(name, side):
        return below[name] if side == 0 else above[name]

    def when_do(condition, act):
        @pl.when(condition)
        def _():
            act()

    def landed(name, ref, recv):
        def wait(part):
            remote(part, part, recv, recv, beside(name, 0)).wait_recv()

        if sizes[name] == 2:
            wait(ref.at[0])
        elif sizes[name] > 2:
            both = jnp.logical_and(below[name], above[name])
            when_do(both, lambda: wait(ref))
            when_do(jnp.logical_not(both), lambda: wait(ref.at[0]))

    def forward(c):
        for side in range(2):

            @pl.when(place["gx"] == by_way_of(side))
            def _(side=side):
                hop_copy(side, c).wait_recv()
                onward_copy(side, c).start()

    def send_bulk(c):
        for side in range(2):
            if c in relayed:
                straight = jnp.logical_and(target("gx", side), jnp.logical_not(middle(side)))
                when_do(straight, lambda: bulk_copy(side, c).start())
                when_do(middle(side), lambda: hop_copy(side, c).start())
            else:
                when_do(target("gx", side), lambda: bulk_copy(side, c).start())

    def y_edges(c):
        lanes = slice(c * chunk, (c + 1) * chunk)
        landed("gx", x_in.at[:, 0, :, span_of(c)], edge_recv.at[c])
        low, high = x_in[0, 0, :, lanes], pltpu.roll(x_in[1, 0, :, lanes], 7, 0)
        for side in range(2):
            turn = (row_index(low.shape) + (8 - Y_EDGE[side])) % 8
            extra = jnp.where(turn % 2 == 1, low, high)
            extra = jnp.where(turn < 6, extra, 0.0)
            y_out[side, 0, :, lanes] = y_out[side, 0, :, lanes] + extra
        for side in range(2):
            when_do(target("gy", side), lambda: y_edge_copy(side, c).start())

    forward_xy, back_xy = mat[0:128, :], mat[128:256, :]
    forward_z, back_z = mat[256:512, :], mat[512:768, :]

    greeted = sum(side[name].astype(jnp.int32) for name in names for side in (below, above))
    greeted = greeted + (1 if detour else 0)
    waiting, edging = list(relayed), list(order)
    for at, c in enumerate(order):
        in_copies[c].wait()
        for start in range(c * chunk, (c + 1) * chunk, STEP):
            lanes = slice(start, start + STEP)
            g00, g11, g22, g01, g02, g12 = [metric[k : k + 1, lanes] for k in range(6)]
            pairs = [split(u[comp, :, :, lanes].reshape(64, STEP)) for comp in range(comps)]
            planes = [
                product(forward_xy, jnp.concatenate([high, low, high, low], axis=0))
                for high, low in pairs
            ]
            grads_z = along_lanes(pairs, forward_z)
            sums, z_pairs = [], []
            for both, grad_z in zip(planes, grads_z):
                grad_x, grad_y = both[:64], both[64:]
                flux_x = g00 * grad_x + g01 * grad_y + g02 * grad_z
                flux_y = g01 * grad_x + g11 * grad_y + g12 * grad_z
                x_high, x_low = split(flux_x)
                y_high, y_low = split(flux_y)
                z_pairs.append(split(g02 * grad_x + g12 * grad_y + g22 * grad_z))
                sums.append(
                    product(back_xy, jnp.concatenate([x_high, y_high, x_low, y_low], axis=0))
                )
            backs_z = along_lanes(z_pairs, back_z)
            weight = jnp.concatenate([scale[0:64, :]] * (STEP // LANES), axis=1)
            ends = ([], [])
            sides = ([], [])
            for comp in range(comps):
                twice = sums[comp]
                terms = twice[:64] + twice[64:] + weight * backs_z[comp]
                terms = terms.reshape(8, 8, STEP)
                local[comp, :, :, lanes] = terms
                for side, plane in enumerate(y_planes([terms[n] for n in range(8)])):
                    sides[side].append(plane)
                    ends[side].append(terms[7 if side == 0 else 0])
            for side in range(2):
                for tile, value in enumerate(pack(ends[side], X_EDGE)):
                    x_out[side, tile, :, lanes] = value
                for tile, value in enumerate(pack(sides[side], Y_EDGE[side])):
                    y_out[side, tile, :, lanes] = value
        if at == 0:
            pl.semaphore_wait(barrier, greeted)
        for side in range(2):
            when_do(target("gx", side), lambda: edge_copy(side, c).start())
            when_do(target("gy", side), lambda: y_bulk_copy(side, c).start())
        if at >= BEHIND:
            send_bulk(order[at - BEHIND])
        if at >= LAG and edging:
            y_edges(edging.pop(0))
        if at >= LAG + 1 and waiting:
            forward(waiting.pop(0))
    for c in order[count - min(BEHIND, count) :]:
        send_bulk(c)
    while waiting or edging:
        if edging:
            y_edges(edging.pop(0))
        if waiting:
            forward(waiting.pop(0))

    def xy_sum(comp, n, lanes):
        value = local[comp, n, :, lanes]
        rows = []
        for side in range(2):
            tile, row = y_seat(side, comp, n)
            rows.append(y_in[side, tile, row : row + 1, lanes])
        if n in (0, 7):
            side = 0 if n == 0 else 1
            tiles = [x_in[side, tile, :, lanes] for tile in range(comps)]
            value = value + unpack(tiles, comp, X_EDGE)
        where = row_index(value.shape)
        return value + jnp.where(where == 0, rows[0], jnp.where(where == 7, rows[1], 0.0))

    def arrived(at):
        members = sets[at]
        span = pl.ds(members[0] * chunk, len(members) * chunk)
        landed("gx", x_in.at[:, 1:, :, span], bulk_recv.at[at])
        landed("gy", y_in.at[:, :, :, span], y_recv.at[at])

    def finish(first, last):
        for comp in range(comps):
            for n in range(8):
                value = xy_sum(comp, n, slice(max(first - LANES, 0), min(last + LANES, total)))
                if first == 0:
                    value = jnp.concatenate([z_in[0, comp, n], value], axis=1)
                if last == total:
                    value = jnp.concatenate([value, z_in[1, comp, n]], axis=1)
                width = value.shape[1]
                before = pltpu.roll(value, 1, 1)[:, LANES:-LANES]
                after = pltpu.roll(value, width - 1, 1)[:, LANES:-LANES]
                position = lax.broadcasted_iota(jnp.int32, before.shape, 1) % 8
                extra = jnp.where(position == 7, after, jnp.where(position == 0, before, 0.0))
                out[comp, n, :, first:last] = value[:, LANES:-LANES] + extra

    def sent(out_ref, in_ref, send, side):
        remote(out_ref.at[side], in_ref.at[side], send.at[side], send.at[side], beside("gz", 0)).wait_send()

    def onward_sent():
        part = relay.at[:, :, pl.ds(0, len(relayed) * chunk)]
        remote(part, part, r_send.at[0], r_send.at[0], beside("gz", 0)).wait_send()

    tiles = total // LANES
    outer = {0, tiles - 1}
    todo, here = set(range(tiles)) - outer, set()
    ends_here = False
    for at, members in enumerate(sets):
        arrived(at)
        for c in members:
            here |= set(range(c * chunk // LANES, (c + 1) * chunk // LANES))
        if outer <= here and not ends_here:
            ends_here = True
            for side in range(2):
                lanes = slice(total - LANES, total) if side == 0 else slice(0, LANES)
                for comp in range(comps):
                    for n in range(8):
                        z_out[side, comp, n] = xy_sum(comp, n, lanes)
                when_do(target("gz", side), lambda: z_copy(side).start())
        ready = sorted(t for t in todo if {t - 1, t, t + 1} <= here)
        todo -= set(ready)
        while ready:
            first = last = ready.pop(0)
            while ready and ready[0] == last + 1:
                last = ready.pop(0)
            finish(first * LANES, (last + 1) * LANES)
    for side in range(2):
        when_do(source("gz", side), lambda: z_copy(side).wait_recv())
    for t in sorted(outer):
        finish(t * LANES, (t + 1) * LANES)

    for side in range(2):
        when_do(target("gx", side), lambda: sent(x_out, x_in, x_send, side))
        when_do(target("gy", side), lambda: sent(y_out, y_in, y_send, side))
        when_do(target("gz", side), lambda: z_copy(side).wait_send())
    if relayed:
        when_do(jnp.logical_or(place["gx"] == 0, place["gx"] == 3), onward_sent)


def local_part(sizes, nodal_scalar_values, geometry):
    comps, _, _, total = nodal_scalar_values.shape
    chunk = min(STEP, total)
    count = total // chunk
    sets = len(chunk_sets(chunk_order(count)))
    matrices, scales = tables()
    f32 = jnp.float32
    dma = pltpu.SemaphoreType.DMA
    any_space = pl.BlockSpec(memory_space=pl.ANY)
    plane = pltpu.VMEM((2, comps, 8, total), f32)
    column = pltpu.VMEM((2, comps, 8, 8, LANES), f32)
    return pl.pallas_call(
        functools.partial(kernel, sizes, chunk),
        out_shape=pltpu.VMEM(nodal_scalar_values.shape, f32),
        in_specs=[any_space] * 4,
        out_specs=pl.BlockSpec(memory_space=pltpu.VMEM),
        scratch_shapes=[
            pltpu.VMEM(nodal_scalar_values.shape, f32),
            pltpu.VMEM(geometry.shape, f32),
            pltpu.VMEM(matrices.shape, jnp.bfloat16),
            pltpu.VMEM(scales.shape, f32),
            pltpu.VMEM((8, total), f32),
            pltpu.VMEM(nodal_scalar_values.shape, f32),
            plane,
            plane,
            plane,
            plane,
            column,
            column,
            pltpu.VMEM((comps - 1, 8, total), f32),
            dma((count,)),
            dma((3,)),
            dma((2,)),
            dma((2,)),
            dma((2,)),
            dma((1,)),
            dma((count,)),
            dma((sets,)),
            dma((sets,)),
            dma((2,)),
            dma((max(count * 3 // 4, 1),)),
        ],
        compiler_params=pltpu.CompilerParams(collective_id=0, has_side_effects=True),
        name="poisson",
    )(nodal_scalar_values, geometry, jnp.asarray(matrices), jnp.asarray(scales))


def solution(mesh):
    return jax.shard_map(
        functools.partial(local_part, dict(mesh.shape)),
        mesh=mesh,
        in_specs=(P(None, "gx", "gy", "gz"), P(None, "gx", "gy", "gz")),
        out_specs=P(None, "gx", "gy", "gz"),
        check_vma=False,
    )
```

```python
import functools

import jax
import jax.numpy as jnp
import numpy as np
from jax import lax
from jax.experimental import pallas as pl
from jax.experimental.pallas import tpu as pltpu
from jax.sharding import PartitionSpec as P

interior_points = [
    -0.8717401485096066,
    -0.5917001814331423,
    -0.2092992179024789,
    0.2092992179024789,
    0.5917001814331423,
    0.8717401485096066,
]
MESH = pl.DeviceIdType.MESH
STEP = 512
LANES = 128
X_FIRST = True
BEHIND = 1
EARLY_BULK = 2
RELAYED = 3
EDGES_FIRST = 2
OUTER_EARLY = 0
X_EDGE = 7
Y_EDGE = (6, 7)


def legendre_seven(point):
    previous = 1.0
    current = point
    for order in range(1, 7):
        following = ((2 * order + 1) * point * current - order * previous) / (order + 1)
        previous = current
        current = following
    return current


def gll_tables():
    degree = 7
    points = [-1.0] + interior_points + [1.0]
    values = [legendre_seven(point) for point in points]
    node_count = degree + 1
    weights = np.array([2.0 / (degree * (degree + 1) * value * value) for value in values])
    derivative = np.zeros((node_count, node_count))
    for row_index in range(node_count):
        for col_index in range(node_count):
            if row_index != col_index:
                derivative[row_index, col_index] = values[row_index] / (
                    values[col_index] * (points[row_index] - points[col_index])
                )
    derivative[0, 0] = -degree * (degree + 1) / 4.0
    derivative[node_count - 1, node_count - 1] = degree * (degree + 1) / 4.0
    return (derivative, weights)


def halves(table):
    table = np.asarray(table, np.float32)
    high = table.astype(jnp.bfloat16)
    low = (table - high.astype(np.float32)).astype(jnp.bfloat16)
    return high, low


def tables():
    derivative, weights = gll_tables()
    eye = np.eye(8)
    plane_weight = np.kron(weights, weights)
    forward_xy = np.concatenate([np.kron(derivative, eye), np.kron(eye, derivative)], axis=0)
    back_xy = np.concatenate([np.kron(derivative.T, eye), np.kron(eye, derivative.T)], axis=1)
    back_xy = back_xy * np.tile(plane_weight, 2)[None, :]
    forward_z = np.kron(np.eye(16), derivative.T)
    back_z = np.kron(np.eye(16), derivative)
    high, low = halves(forward_xy)
    forward_xy = np.concatenate([high, high, low, low], axis=1)
    high, low = halves(back_xy)
    back_xy = np.concatenate(
        [np.concatenate([high, high], axis=1), np.concatenate([low, low], axis=1)], axis=0
    )
    high, low = halves(forward_z)
    forward_z = np.tile(np.concatenate([high, low], axis=1), (2, 1))
    high, low = halves(back_z)
    back_z = np.tile(np.concatenate([high, low], axis=1), (2, 1))
    matrices = np.concatenate([forward_xy, back_xy, forward_z, back_z], axis=0)
    plane = np.repeat(plane_weight[:, None], LANES, axis=1)
    along = np.repeat(np.tile(weights, LANES // 8)[None, :], 8, axis=0)
    scales = np.concatenate([plane, along], axis=0).astype(np.float32)
    return matrices, scales


def row_index(shape):
    return lax.broadcasted_iota(jnp.int32, shape, 0)


def pack(planes, edge):
    first, second, third = planes
    turn = (row_index(first.shape) + (8 - edge)) % 8
    own = turn < 2
    second_edge = jnp.logical_and(turn >= 2, turn < 4)
    third_edge = jnp.logical_and(turn >= 4, turn < 6)
    edges = jnp.where(
        second_edge,
        pltpu.roll(second, 2, 0),
        jnp.where(third_edge, pltpu.roll(third, 4, 0), first),
    )
    return [
        edges,
        jnp.where(own, pltpu.roll(first, 6, 0), second),
        jnp.where(own, pltpu.roll(first, 4, 0), third),
    ]


def unpack(tiles, comp, edge):
    turn = (row_index(tiles[0].shape) + (8 - edge)) % 8
    if comp:
        return jnp.where(turn < 2, pltpu.roll(tiles[0], 8 - 2 * comp, 0), tiles[comp])
    from_second = jnp.logical_and(turn >= 2, turn < 4)
    from_third = jnp.logical_and(turn >= 4, turn < 6)
    return jnp.where(
        from_second,
        pltpu.roll(tiles[1], 2, 0),
        jnp.where(from_third, pltpu.roll(tiles[2], 4, 0), tiles[0]),
    )


def y_planes(terms):
    turn = (row_index(terms[0].shape) + 1) % 8

    def gather(four):
        return jnp.where(
            turn < 2,
            four[0],
            jnp.where(
                turn < 4,
                pltpu.roll(four[1], 2, 0),
                jnp.where(turn < 6, pltpu.roll(four[2], 4, 0), pltpu.roll(four[3], 6, 0)),
            ),
        )

    low, high = gather(terms[:4]), pltpu.roll(gather(terms[4:]), 1, 0)
    even = turn % 2 == 0
    return jnp.where(even, low, high), jnp.where(even, high, low)


def y_seat(side, comp, n):
    edge = Y_EDGE[side]
    row = (2 * n + 7 + side) % 8 if n < 4 else 2 * (n - 4) + side
    turn = (row - edge) % 8
    if turn < 2:
        return 0, (row + 2 * comp) % 8
    if comp:
        return comp, row
    if turn < 6:
        return turn // 2, (row - 2 * (turn // 2)) % 8
    return 0, row


def split(value):
    high = value.astype(jnp.bfloat16)
    low = (value - high.astype(jnp.float32)).astype(jnp.bfloat16)
    return high, low


def product(left, right):
    return jnp.dot(left, right, preferred_element_type=jnp.float32)


def along_lanes(pairs, table):
    rows, width = pairs[0][0].shape
    spans = [slice(start, start + LANES) for start in range(0, width, LANES)]
    stacked = [
        jnp.concatenate([high[:, span], low[:, span]], axis=1)
        for high, low in pairs
        for span in spans
    ]
    twice = product(jnp.concatenate(stacked, axis=0), table)
    once = twice[:, :LANES] + twice[:, LANES:]
    pieces = [once[at * rows : (at + 1) * rows] for at in range(len(stacked))]
    return [
        jnp.concatenate(pieces[at : at + len(spans)], axis=1)
        for at in range(0, len(pieces), len(spans))
    ]


def chunk_spans(total):
    if total % STEP or total < 2 * STEP:
        return [(0, total)]
    widths = [STEP // 2] + [STEP] * (total // STEP - 1) + [STEP // 2]
    starts = [sum(widths[:at]) for at in range(len(widths))]
    return list(zip(starts, widths))


def chunk_order(count):
    return [0] + ([count - 1] if count > 1 else []) + list(range(1, count - 1))


def relayed_chunks(spans):
    total = sum(width for _, width in spans)
    chosen, lanes = [], 0
    for c in chunk_order(len(spans)):
        if (lanes + spans[c][1]) * 4 <= total * RELAYED:
            chosen.append(c)
            lanes += spans[c][1]
    return chosen


def kernel(
    sizes,
    spans,
    u_hbm,
    geo_hbm,
    mat_hbm,
    scale_hbm,
    out,
    u,
    geo,
    mat,
    scale,
    metric,
    local,
    x_out,
    y_out,
    x_in,
    y_in,
    z_out,
    z_in,
    relay,
    in_sem,
    const_sem,
    x_send,
    y_send,
    z_send,
    r_send,
    edge_recv,
    bulk_recv,
    y_recv,
    z_recv,
    r_recv,
):
    comps, _, _, total = u.shape
    count = len(spans)
    order = chunk_order(count)
    names = ("gx", "gy", "gz")
    place = {name: lax.axis_index(name) for name in names}
    below = {name: place[name] > 0 for name in names}
    above = {name: place[name] < sizes[name] - 1 for name in names}

    const_copies = [
        pltpu.make_async_copy(mat_hbm, mat, const_sem.at[0]),
        pltpu.make_async_copy(scale_hbm, scale, const_sem.at[1]),
        pltpu.make_async_copy(geo_hbm, geo, const_sem.at[2]),
    ]
    for copy in const_copies:
        copy.start()
    in_copies = {}
    loads = [[c] for c in order[:2]] + ([sorted(order[2:])] if count > 2 else [])
    for at, members in enumerate(loads):
        span = pl.ds(spans[members[0]][0], sum(spans[c][1] for c in members))
        in_copies[members[0]] = pltpu.make_async_copy(
            u_hbm.at[:, :, :, span], u.at[:, :, :, span], in_sem.at[at]
        )
        in_copies[members[0]].start()

    barrier = pltpu.get_barrier_semaphore()
    for name in names:
        for there, by in ((below[name], -1), (above[name], 1)):

            @pl.when(there)
            def _(name=name, by=by):
                pl.semaphore_signal(
                    barrier, inc=1, device_id={name: place[name] + by}, device_id_type=MESH
                )

    detour = sizes["gx"] == 4
    relayed = relayed_chunks(spans) if detour else []
    opposite = lax.rem(place["gx"] + 2, 4)
    if detour:
        pl.semaphore_signal(barrier, inc=1, device_id={"gx": opposite}, device_id_type=MESH)

    for side in range(2):
        there = below if side == 0 else above

        @pl.when(jnp.logical_not(there["gx"]))
        def _(side=side):
            x_in[side] = jnp.zeros(x_in.shape[1:], jnp.float32)

        @pl.when(jnp.logical_not(there["gy"]))
        def _(side=side):
            y_in[side] = jnp.zeros(y_in.shape[1:], jnp.float32)

        @pl.when(jnp.logical_not(there["gz"]))
        def _(side=side):
            z_in[side] = jnp.zeros(z_in.shape[1:], jnp.float32)

    for copy in const_copies:
        copy.wait()

    rows = jnp.concatenate(
        [geo[k, 0] for k in range(6)] + [jnp.zeros((2, geo.shape[-1]), jnp.float32)], axis=0
    )
    lane = lax.broadcasted_iota(jnp.int32, (8, LANES), 1)
    for tile in range(total // LANES):
        first = tile * (LANES // 8)
        block = rows[:, first // LANES * LANES : first // LANES * LANES + LANES]
        spread = jnp.take_along_axis(block, lane // 8 + first % LANES, axis=1)
        metric[:, tile * LANES : (tile + 1) * LANES] = spread * scale[64:72, :]

    def span_of(c):
        return pl.ds(*spans[c])

    def beside(name, side):
        return {name: place[name] + (1 if side == 0 else -1)}

    def remote(source, target, send, recv, device):
        return pltpu.make_async_remote_copy(
            source, target, send, recv, device_id=device, device_id_type=MESH
        )

    def edge_copy(side, c):
        at = (side, 0, slice(None), span_of(c))
        return remote(
            x_out.at[at], x_in.at[at], x_send.at[0], edge_recv.at[c], beside("gx", side)
        )

    def bulk_copy(side, c):
        at = (side, slice(1, None), slice(None), span_of(c))
        return remote(
            x_out.at[at],
            x_in.at[at],
            x_send.at[0],
            bulk_recv.at[c],
            beside("gx", side),
        )

    def y_edge_copy(side, c):
        at = (side, 0, slice(None), span_of(c))
        return remote(
            y_out.at[at], y_in.at[at], y_send.at[0], y_recv.at[c], beside("gy", side)
        )

    def y_bulk_copy(side, c):
        at = (side, slice(1, None), slice(None), span_of(c))
        return remote(
            y_out.at[at], y_in.at[at], y_send.at[0], y_recv.at[c], beside("gy", side)
        )

    def z_copy(side):
        return remote(
            z_out.at[side], z_in.at[side], z_send.at[0], z_recv.at[0], beside("gz", side)
        )

    def middle(side):
        return place["gx"] == 1 + side

    def by_way_of(side):
        return 3 * (1 - side) if X_FIRST else 3 * side

    def hop_copy(side, c):
        return remote(
            x_out.at[side, 1:, :, span_of(c)],
            relay.at[:, :, span_of(c)],
            x_send.at[0],
            r_recv.at[relayed.index(c)],
            {"gx": by_way_of(side)},
        )

    def onward_copy(side, c):
        return remote(
            relay.at[:, :, span_of(c)],
            x_in.at[side, 1:, :, span_of(c)],
            r_send.at[0],
            bulk_recv.at[c],
            {"gx": 2 - side},
        )

    def target(name, side):
        return above[name] if side == 0 else below[name]

    def source(name, side):
        return below[name] if side == 0 else above[name]

    def when_do(condition, act):
        @pl.when(condition)
        def _():
            act()

    def landed(name, ref, recv):
        def wait(part):
            remote(part, part, recv, recv, beside(name, 0)).wait_recv()

        if sizes[name] == 2:
            wait(ref.at[0])
        elif sizes[name] > 2:
            both = jnp.logical_and(below[name], above[name])
            when_do(both, lambda: wait(ref))
            when_do(jnp.logical_not(both), lambda: wait(ref.at[0]))

    def forward(c):
        for side in range(2):

            @pl.when(place["gx"] == by_way_of(side))
            def _(side=side):
                hop_copy(side, c).wait_recv()
                onward_copy(side, c).start()

    def straight(side):
        if detour:
            return jnp.logical_and(target("gx", side), jnp.logical_not(middle(side)))
        return target("gx", side)

    def send_outer(c):
        for side in range(2):
            when_do(straight(side), lambda: bulk_copy(side, c).start())

    def send_inner(c):
        for side in range(2):
            if c in relayed:
                when_do(middle(side), lambda: hop_copy(side, c).start())
            elif detour:
                when_do(middle(side), lambda: bulk_copy(side, c).start())

    def y_edges(c):
        lanes = slice(spans[c][0], sum(spans[c]))
        landed("gx", x_in.at[:, 0, :, span_of(c)], edge_recv.at[c])
        low, high = x_in[0, 0, :, lanes], pltpu.roll(x_in[1, 0, :, lanes], 7, 0)
        for side in range(2):
            turn = (row_index(low.shape) + (8 - Y_EDGE[side])) % 8
            extra = jnp.where(turn % 2 == 1, low, high)
            extra = jnp.where(turn < 6, extra, 0.0)
            y_out[side, 0, :, lanes] = y_out[side, 0, :, lanes] + extra
        for side in range(2):
            when_do(target("gy", side), lambda: y_edge_copy(side, c).start())

    forward_xy, back_xy = mat[0:128, :], mat[128:256, :]
    forward_z, back_z = mat[256:512, :], mat[512:768, :]

    greeted = sum(side[name].astype(jnp.int32) for name in names for side in (below, above))
    greeted = greeted + (1 if detour else 0)
    waiting, edging = list(relayed), list(order)
    for at, c in enumerate(order):
        if c in in_copies:
            in_copies[c].wait()
        step = spans[c][1]
        for start in (spans[c][0],):
            lanes = slice(start, start + step)
            g00, g11, g22, g01, g02, g12 = [metric[k : k + 1, lanes] for k in range(6)]
            pairs = [split(u[comp, :, :, lanes].reshape(64, step)) for comp in range(comps)]
            planes = [
                product(forward_xy, jnp.concatenate([high, low, high, low], axis=0))
                for high, low in pairs
            ]
            grads_z = along_lanes(pairs, forward_z)
            sums, z_pairs = [], []
            for both, grad_z in zip(planes, grads_z):
                grad_x, grad_y = both[:64], both[64:]
                flux_x = g00 * grad_x + g01 * grad_y + g02 * grad_z
                flux_y = g01 * grad_x + g11 * grad_y + g12 * grad_z
                x_high, x_low = split(flux_x)
                y_high, y_low = split(flux_y)
                z_pairs.append(split(g02 * grad_x + g12 * grad_y + g22 * grad_z))
                sums.append(
                    product(back_xy, jnp.concatenate([x_high, y_high, x_low, y_low], axis=0))
                )
            backs_z = along_lanes(z_pairs, back_z)
            weight = jnp.concatenate([scale[0:64, :]] * (step // LANES), axis=1)
            ends = ([], [])
            sides = ([], [])
            for comp in range(comps):
                twice = sums[comp]
                terms = twice[:64] + twice[64:] + weight * backs_z[comp]
                terms = terms.reshape(8, 8, step)
                local[comp, :, :, lanes] = terms
                for side, plane in enumerate(y_planes([terms[n] for n in range(8)])):
                    sides[side].append(plane)
                    ends[side].append(terms[7 if side == 0 else 0])
            for side in range(2):
                for tile, value in enumerate(pack(ends[side], X_EDGE)):
                    x_out[side, tile, :, lanes] = value
                for tile, value in enumerate(pack(sides[side], Y_EDGE[side])):
                    y_out[side, tile, :, lanes] = value
        if at == 0:
            pl.semaphore_wait(barrier, greeted)
        for side in range(2):
            when_do(straight(side), lambda: edge_copy(side, c).start())
        for side in range(2):
            if detour:
                when_do(middle(side), lambda: edge_copy(side, c).start())
            when_do(target("gy", side), lambda: y_bulk_copy(side, c).start())
        if c in relayed:
            send_inner(c)
        if 0 <= at - BEHIND < EARLY_BULK:
            send_outer(order[at - BEHIND])
    for c in order[min(EARLY_BULK, max(count - BEHIND, 0)) :]:
        send_outer(c)
    for c in order:
        if c not in relayed:
            send_inner(c)
    while waiting or edging:
        if edging:
            y_edges(edging.pop(0))
        if waiting and count - len(edging) >= EDGES_FIRST:
            forward(waiting.pop(0))

    def xy_sum(comp, n, lanes):
        value = local[comp, n, :, lanes]
        rows = []
        for side in range(2):
            tile, row = y_seat(side, comp, n)
            rows.append(y_in[side, tile, row : row + 1, lanes])
        if n in (0, 7):
            side = 0 if n == 0 else 1
            tiles = [x_in[side, tile, :, lanes] for tile in range(comps)]
            value = value + unpack(tiles, comp, X_EDGE)
        where = row_index(value.shape)
        return value + jnp.where(where == 0, rows[0], jnp.where(where == 7, rows[1], 0.0))

    def arrived(c):
        landed("gx", x_in.at[:, 1:, :, span_of(c)], bulk_recv.at[c])
        landed("gy", y_in.at[:, :, :, span_of(c)], y_recv.at[c])

    def finish(first, last):
        for comp in range(comps):
            for n in range(8):
                value = xy_sum(comp, n, slice(max(first - LANES, 0), min(last + LANES, total)))
                if first == 0:
                    value = jnp.concatenate([z_in[0, comp, n], value], axis=1)
                if last == total:
                    value = jnp.concatenate([value, z_in[1, comp, n]], axis=1)
                width = value.shape[1]
                before = pltpu.roll(value, 1, 1)[:, LANES:-LANES]
                after = pltpu.roll(value, width - 1, 1)[:, LANES:-LANES]
                position = lax.broadcasted_iota(jnp.int32, before.shape, 1) % 8
                extra = jnp.where(position == 7, after, jnp.where(position == 0, before, 0.0))
                out[comp, n, :, first:last] = value[:, LANES:-LANES] + extra

    def sent(name, ref, send):
        def wait(part):
            remote(part, part, send, send, beside(name, 0)).wait_send()

        if sizes[name] == 2:
            wait(ref.at[0])
        elif sizes[name] > 2:
            both = jnp.logical_and(below[name], above[name])
            when_do(both, lambda: wait(ref))
            when_do(jnp.logical_not(both), lambda: wait(ref.at[0]))

    def onward_sent():
        part = relay.at[:, :, pl.ds(0, sum(spans[c][1] for c in relayed))]
        remote(part, part, r_send.at[0], r_send.at[0], beside("gz", 0)).wait_send()

    def finish_outer():
        landed("gz", z_in, z_recv.at[0])
        for t in sorted(outer):
            finish(t * LANES, (t + 1) * LANES)

    tiles = total // LANES
    outer = {0, tiles - 1}
    todo, here = set(range(tiles)) - outer, set()
    ends_here = False
    for at, c in enumerate(order):
        if at == count - 1 - OUTER_EARLY and at >= 2:
            finish_outer()
        arrived(c)
        here |= set(range(spans[c][0] // LANES, sum(spans[c]) // LANES))
        if outer <= here and not ends_here:
            ends_here = True
            for side in range(2):
                lanes = slice(total - LANES, total) if side == 0 else slice(0, LANES)
                for comp in range(comps):
                    for n in range(8):
                        z_out[side, comp, n] = xy_sum(comp, n, lanes)
                when_do(target("gz", side), lambda: z_copy(side).start())
        ready = sorted(t for t in todo if {t - 1, t, t + 1} <= here)
        todo -= set(ready)
        while ready:
            first = last = ready.pop(0)
            while ready and ready[0] == last + 1:
                last = ready.pop(0)
            finish(first * LANES, (last + 1) * LANES)
    if count - 1 - OUTER_EARLY not in range(2, count):
        finish_outer()

    sent("gx", x_out, x_send.at[0])
    sent("gy", y_out, y_send.at[0])
    sent("gz", z_out, z_send.at[0])
    if relayed:
        when_do(jnp.logical_or(place["gx"] == 0, place["gx"] == 3), onward_sent)


def local_part(sizes, nodal_scalar_values, geometry):
    comps, _, _, total = nodal_scalar_values.shape
    spans = chunk_spans(total)
    count = len(spans)
    matrices, scales = tables()
    f32 = jnp.float32
    dma = pltpu.SemaphoreType.DMA
    any_space = pl.BlockSpec(memory_space=pl.ANY)
    plane = pltpu.VMEM((2, comps, 8, total), f32)
    column = pltpu.VMEM((2, comps, 8, 8, LANES), f32)
    return pl.pallas_call(
        functools.partial(kernel, sizes, spans),
        out_shape=pltpu.VMEM(nodal_scalar_values.shape, f32),
        in_specs=[any_space] * 4,
        out_specs=pl.BlockSpec(memory_space=pltpu.VMEM),
        scratch_shapes=[
            pltpu.VMEM(nodal_scalar_values.shape, f32),
            pltpu.VMEM(geometry.shape, f32),
            pltpu.VMEM(matrices.shape, jnp.bfloat16),
            pltpu.VMEM(scales.shape, f32),
            pltpu.VMEM((8, total), f32),
            pltpu.VMEM(nodal_scalar_values.shape, f32),
            plane,
            plane,
            plane,
            plane,
            column,
            column,
            pltpu.VMEM((comps - 1, 8, total), f32),
            dma((min(count, 3),)),
            dma((3,)),
            dma((1,)),
            dma((1,)),
            dma((1,)),
            dma((1,)),
            dma((count,)),
            dma((count,)),
            dma((count,)),
            dma((1,)),
            dma((max(len(relayed_chunks(spans)), 1),)),
        ],
        compiler_params=pltpu.CompilerParams(collective_id=0, has_side_effects=True),
        name="poisson",
    )(nodal_scalar_values, geometry, jnp.asarray(matrices), jnp.asarray(scales))


def solution(mesh):
    return jax.shard_map(
        functools.partial(local_part, dict(mesh.shape)),
        mesh=mesh,
        in_specs=(P(None, "gx", "gy", "gz"), P(None, "gx", "gy", "gz")),
        out_specs=P(None, "gx", "gy", "gz"),
        check_vma=False,
    )
```

```python
import functools

import jax
import jax.numpy as jnp
import numpy as np
from jax import lax
from jax.experimental import pallas as pl
from jax.experimental.pallas import tpu as pltpu
from jax.sharding import PartitionSpec as P

interior_points = [
    -0.8717401485096066,
    -0.5917001814331423,
    -0.2092992179024789,
    0.2092992179024789,
    0.5917001814331423,
    0.8717401485096066,
]
MESH = pl.DeviceIdType.MESH
STEP = 512
LANES = 128
X_FIRST = True
BEHIND = 1
EARLY_BULK = 2
RELAYED = 3
EDGES_FIRST = 2
OUTER_EARLY = 0
INNER = 256
X_EDGE = 7
Y_EDGE = (6, 7)


def legendre_seven(point):
    previous = 1.0
    current = point
    for order in range(1, 7):
        following = ((2 * order + 1) * point * current - order * previous) / (order + 1)
        previous = current
        current = following
    return current


def gll_tables():
    degree = 7
    points = [-1.0] + interior_points + [1.0]
    values = [legendre_seven(point) for point in points]
    node_count = degree + 1
    weights = np.array([2.0 / (degree * (degree + 1) * value * value) for value in values])
    derivative = np.zeros((node_count, node_count))
    for row_index in range(node_count):
        for col_index in range(node_count):
            if row_index != col_index:
                derivative[row_index, col_index] = values[row_index] / (
                    values[col_index] * (points[row_index] - points[col_index])
                )
    derivative[0, 0] = -degree * (degree + 1) / 4.0
    derivative[node_count - 1, node_count - 1] = degree * (degree + 1) / 4.0
    return (derivative, weights)


def halves(table):
    table = np.asarray(table, np.float32)
    high = table.astype(jnp.bfloat16)
    low = (table - high.astype(np.float32)).astype(jnp.bfloat16)
    return high, low


def tables():
    derivative, weights = gll_tables()
    eye = np.eye(8)
    plane_weight = np.kron(weights, weights)
    forward_xy = np.concatenate([np.kron(derivative, eye), np.kron(eye, derivative)], axis=0)
    back_xy = np.concatenate([np.kron(derivative.T, eye), np.kron(eye, derivative.T)], axis=1)
    back_xy = back_xy * np.tile(plane_weight, 2)[None, :]
    forward_z = np.kron(np.eye(16), derivative.T)
    back_z = np.kron(np.eye(16), derivative)
    high, low = halves(forward_xy)
    forward_xy = np.concatenate([high, high, low, low], axis=1)
    high, low = halves(back_xy)
    back_xy = np.concatenate(
        [np.concatenate([high, high], axis=1), np.concatenate([low, low], axis=1)], axis=0
    )
    high, low = halves(forward_z)
    forward_z = np.tile(np.concatenate([high, low], axis=1), (2, 1))
    high, low = halves(back_z)
    back_z = np.tile(np.concatenate([high, low], axis=1), (2, 1))
    matrices = np.concatenate([forward_xy, back_xy, forward_z, back_z], axis=0)
    plane = np.repeat(plane_weight[:, None], LANES, axis=1)
    along = np.repeat(np.tile(weights, LANES // 8)[None, :], 8, axis=0)
    scales = np.concatenate([plane, along], axis=0).astype(np.float32)
    return matrices, scales


def row_index(shape):
    return lax.broadcasted_iota(jnp.int32, shape, 0)


def pack(planes, edge):
    first, second, third = planes
    turn = (row_index(first.shape) + (8 - edge)) % 8
    own = turn < 2
    second_edge = jnp.logical_and(turn >= 2, turn < 4)
    third_edge = jnp.logical_and(turn >= 4, turn < 6)
    edges = jnp.where(
        second_edge,
        pltpu.roll(second, 2, 0),
        jnp.where(third_edge, pltpu.roll(third, 4, 0), first),
    )
    return [
        edges,
        jnp.where(own, pltpu.roll(first, 6, 0), second),
        jnp.where(own, pltpu.roll(first, 4, 0), third),
    ]


def unpack(tiles, comp, edge):
    turn = (row_index(tiles[0].shape) + (8 - edge)) % 8
    if comp:
        return jnp.where(turn < 2, pltpu.roll(tiles[0], 8 - 2 * comp, 0), tiles[comp])
    from_second = jnp.logical_and(turn >= 2, turn < 4)
    from_third = jnp.logical_and(turn >= 4, turn < 6)
    return jnp.where(
        from_second,
        pltpu.roll(tiles[1], 2, 0),
        jnp.where(from_third, pltpu.roll(tiles[2], 4, 0), tiles[0]),
    )


def y_planes(terms):
    turn = (row_index(terms[0].shape) + 1) % 8

    def gather(four):
        return jnp.where(
            turn < 2,
            four[0],
            jnp.where(
                turn < 4,
                pltpu.roll(four[1], 2, 0),
                jnp.where(turn < 6, pltpu.roll(four[2], 4, 0), pltpu.roll(four[3], 6, 0)),
            ),
        )

    low, high = gather(terms[:4]), pltpu.roll(gather(terms[4:]), 1, 0)
    even = turn % 2 == 0
    return jnp.where(even, low, high), jnp.where(even, high, low)


def y_seat(side, comp, n):
    edge = Y_EDGE[side]
    row = (2 * n + 7 + side) % 8 if n < 4 else 2 * (n - 4) + side
    turn = (row - edge) % 8
    if turn < 2:
        return 0, (row + 2 * comp) % 8
    if comp:
        return comp, row
    if turn < 6:
        return turn // 2, (row - 2 * (turn // 2)) % 8
    return 0, row


def split(value):
    high = value.astype(jnp.bfloat16)
    low = (value - high.astype(jnp.float32)).astype(jnp.bfloat16)
    return high, low


def product(left, right):
    return jnp.dot(left, right, preferred_element_type=jnp.float32)


def along_lanes(pairs, table):
    rows, width = pairs[0][0].shape
    spans = [slice(start, start + LANES) for start in range(0, width, LANES)]
    stacked = [
        jnp.concatenate([high[:, span], low[:, span]], axis=1)
        for high, low in pairs
        for span in spans
    ]
    twice = product(jnp.concatenate(stacked, axis=0), table)
    once = twice[:, :LANES] + twice[:, LANES:]
    pieces = [once[at * rows : (at + 1) * rows] for at in range(len(stacked))]
    return [
        jnp.concatenate(pieces[at : at + len(spans)], axis=1)
        for at in range(0, len(pieces), len(spans))
    ]


def chunk_spans(total):
    if total % STEP or total < 2 * STEP:
        return [(0, total)]
    widths = [STEP // 2] + [STEP] * (total // STEP - 1) + [STEP // 2]
    starts = [sum(widths[:at]) for at in range(len(widths))]
    return list(zip(starts, widths))


def chunk_order(count):
    return [0] + ([count - 1] if count > 1 else []) + list(range(1, count - 1))


def relayed_chunks(spans):
    total = sum(width for _, width in spans)
    chosen, lanes = [], 0
    for c in chunk_order(len(spans)):
        if (lanes + spans[c][1]) * 4 <= total * RELAYED:
            chosen.append(c)
            lanes += spans[c][1]
    return chosen


def kernel(
    sizes,
    spans,
    u_hbm,
    geo_hbm,
    mat_hbm,
    scale_hbm,
    out,
    u,
    geo,
    mat,
    scale,
    metric,
    local,
    x_out,
    y_out,
    x_in,
    y_in,
    z_out,
    z_in,
    relay,
    in_sem,
    const_sem,
    x_send,
    y_send,
    z_send,
    r_send,
    edge_recv,
    bulk_recv,
    y_recv,
    y_bulk_recv,
    z_recv,
    r_recv,
):
    comps, _, _, total = u.shape
    count = len(spans)
    order = chunk_order(count)
    names = ("gx", "gy", "gz")
    place = {name: lax.axis_index(name) for name in names}
    below = {name: place[name] > 0 for name in names}
    above = {name: place[name] < sizes[name] - 1 for name in names}

    const_copies = [
        pltpu.make_async_copy(mat_hbm, mat, const_sem.at[0]),
        pltpu.make_async_copy(scale_hbm, scale, const_sem.at[1]),
        pltpu.make_async_copy(geo_hbm, geo, const_sem.at[2]),
    ]
    for copy in const_copies:
        copy.start()
    in_copies = {}
    loads = [[c] for c in order[:2]] + ([sorted(order[2:])] if count > 2 else [])
    for at, members in enumerate(loads):
        span = pl.ds(spans[members[0]][0], sum(spans[c][1] for c in members))
        in_copies[members[0]] = pltpu.make_async_copy(
            u_hbm.at[:, :, :, span], u.at[:, :, :, span], in_sem.at[at]
        )
        in_copies[members[0]].start()

    barrier = pltpu.get_barrier_semaphore()
    for name in names:
        for there, by in ((below[name], -1), (above[name], 1)):

            @pl.when(there)
            def _(name=name, by=by):
                pl.semaphore_signal(
                    barrier, inc=1, device_id={name: place[name] + by}, device_id_type=MESH
                )

    detour = sizes["gx"] == 4
    relayed = relayed_chunks(spans) if detour else []
    opposite = lax.rem(place["gx"] + 2, 4)
    if detour:
        pl.semaphore_signal(barrier, inc=1, device_id={"gx": opposite}, device_id_type=MESH)

    for side in range(2):
        there = below if side == 0 else above

        @pl.when(jnp.logical_not(there["gx"]))
        def _(side=side):
            x_in[side] = jnp.zeros(x_in.shape[1:], jnp.float32)

        @pl.when(jnp.logical_not(there["gy"]))
        def _(side=side):
            y_in[side] = jnp.zeros(y_in.shape[1:], jnp.float32)

        @pl.when(jnp.logical_not(there["gz"]))
        def _(side=side):
            z_in[side] = jnp.zeros(z_in.shape[1:], jnp.float32)

    for copy in const_copies:
        copy.wait()

    rows = jnp.concatenate(
        [geo[k, 0] for k in range(6)] + [jnp.zeros((2, geo.shape[-1]), jnp.float32)], axis=0
    )
    lane = lax.broadcasted_iota(jnp.int32, (8, LANES), 1)
    for tile in range(total // LANES):
        first = tile * (LANES // 8)
        block = rows[:, first // LANES * LANES : first // LANES * LANES + LANES]
        spread = jnp.take_along_axis(block, lane // 8 + first % LANES, axis=1)
        metric[:, tile * LANES : (tile + 1) * LANES] = spread * scale[64:72, :]

    def span_of(c):
        return pl.ds(*spans[c])

    def beside(name, side):
        return {name: place[name] + (1 if side == 0 else -1)}

    def remote(source, target, send, recv, device):
        return pltpu.make_async_remote_copy(
            source, target, send, recv, device_id=device, device_id_type=MESH
        )

    def edge_copy(side, c):
        at = (side, 0, slice(None), span_of(c))
        return remote(
            x_out.at[at], x_in.at[at], x_send.at[0], edge_recv.at[c], beside("gx", side)
        )

    def bulk_copy(side, c):
        at = (side, slice(1, None), slice(None), span_of(c))
        return remote(
            x_out.at[at],
            x_in.at[at],
            x_send.at[0],
            bulk_recv.at[c],
            beside("gx", side),
        )

    def y_edge_copy(side, c):
        at = (side, 0, slice(None), span_of(c))
        return remote(
            y_out.at[at], y_in.at[at], y_send.at[0], y_recv.at[c], beside("gy", side)
        )

    def y_bulk_copy(side, c):
        at = (side, slice(1, None), slice(None), span_of(c))
        return remote(
            y_out.at[at], y_in.at[at], y_send.at[0], y_bulk_recv.at[0], beside("gy", side)
        )

    def z_copy(side):
        return remote(
            z_out.at[side], z_in.at[side], z_send.at[0], z_recv.at[side], beside("gz", side)
        )

    def middle(side):
        return place["gx"] == 1 + side

    def by_way_of(side):
        return 3 * (1 - side) if X_FIRST else 3 * side

    def hop_copy(side, c):
        return remote(
            x_out.at[side, 1:, :, span_of(c)],
            relay.at[:, :, span_of(c)],
            x_send.at[0],
            r_recv.at[relayed.index(c)],
            {"gx": by_way_of(side)},
        )

    def onward_copy(side, c):
        return remote(
            relay.at[:, :, span_of(c)],
            x_in.at[side, 1:, :, span_of(c)],
            r_send.at[0],
            bulk_recv.at[c],
            {"gx": 2 - side},
        )

    def target(name, side):
        return above[name] if side == 0 else below[name]

    def source(name, side):
        return below[name] if side == 0 else above[name]

    def when_do(condition, act):
        @pl.when(condition)
        def _():
            act()

    def landed(name, ref, recv):
        def wait(part):
            remote(part, part, recv, recv, beside(name, 0)).wait_recv()

        if sizes[name] == 2:
            wait(ref.at[0])
        elif sizes[name] > 2:
            both = jnp.logical_and(below[name], above[name])
            when_do(both, lambda: wait(ref))
            when_do(jnp.logical_not(both), lambda: wait(ref.at[0]))

    def forward(c):
        for side in range(2):

            @pl.when(place["gx"] == by_way_of(side))
            def _(side=side):
                hop_copy(side, c).wait_recv()
                onward_copy(side, c).start()

    def straight(side):
        if detour:
            return jnp.logical_and(target("gx", side), jnp.logical_not(middle(side)))
        return target("gx", side)

    def send_outer(c):
        for side in range(2):
            when_do(straight(side), lambda: bulk_copy(side, c).start())

    def send_inner(c):
        for side in range(2):
            if c in relayed:
                when_do(middle(side), lambda: hop_copy(side, c).start())
            elif detour:
                when_do(middle(side), lambda: bulk_copy(side, c).start())

    def y_edges(c):
        lanes = slice(spans[c][0], sum(spans[c]))
        landed("gx", x_in.at[:, 0, :, span_of(c)], edge_recv.at[c])
        low, high = x_in[0, 0, :, lanes], pltpu.roll(x_in[1, 0, :, lanes], 7, 0)
        for side in range(2):
            turn = (row_index(low.shape) + (8 - Y_EDGE[side])) % 8
            extra = jnp.where(turn % 2 == 1, low, high)
            extra = jnp.where(turn < 6, extra, 0.0)
            y_out[side, 0, :, lanes] = y_out[side, 0, :, lanes] + extra
        for side in range(2):
            when_do(target("gy", side), lambda: y_edge_copy(side, c).start())

    forward_xy, back_xy = mat[0:128, :], mat[128:256, :]
    forward_z, back_z = mat[256:512, :], mat[512:768, :]

    greeted = sum(side[name].astype(jnp.int32) for name in names for side in (below, above))
    greeted = greeted + (1 if detour else 0)
    waiting, edging = list(relayed), list(order)
    for at, c in enumerate(order):
        if c in in_copies:
            in_copies[c].wait()
        step = spans[c][1]
        for start in (spans[c][0],):
            lanes = slice(start, start + step)
            g00, g11, g22, g01, g02, g12 = [metric[k : k + 1, lanes] for k in range(6)]
            pairs = [split(u[comp, :, :, lanes].reshape(64, step)) for comp in range(comps)]
            planes = [
                product(forward_xy, jnp.concatenate([high, low, high, low], axis=0))
                for high, low in pairs
            ]
            grads_z = along_lanes(pairs, forward_z)
            sums, z_pairs = [], []
            for both, grad_z in zip(planes, grads_z):
                grad_x, grad_y = both[:64], both[64:]
                flux_x = g00 * grad_x + g01 * grad_y + g02 * grad_z
                flux_y = g01 * grad_x + g11 * grad_y + g12 * grad_z
                x_high, x_low = split(flux_x)
                y_high, y_low = split(flux_y)
                z_pairs.append(split(g02 * grad_x + g12 * grad_y + g22 * grad_z))
                sums.append(
                    product(back_xy, jnp.concatenate([x_high, y_high, x_low, y_low], axis=0))
                )
            backs_z = along_lanes(z_pairs, back_z)
            weight = jnp.concatenate([scale[0:64, :]] * (step // LANES), axis=1)
            ends = ([], [])
            sides = ([], [])
            for comp in range(comps):
                twice = sums[comp]
                terms = twice[:64] + twice[64:] + weight * backs_z[comp]
                terms = terms.reshape(8, 8, step)
                local[comp, :, :, lanes] = terms
                for side, plane in enumerate(y_planes([terms[n] for n in range(8)])):
                    sides[side].append(plane)
                    ends[side].append(terms[7 if side == 0 else 0])
            for side in range(2):
                for tile, value in enumerate(pack(ends[side], X_EDGE)):
                    x_out[side, tile, :, lanes] = value
                for tile, value in enumerate(pack(sides[side], Y_EDGE[side])):
                    y_out[side, tile, :, lanes] = value
        if at == 0:
            pl.semaphore_wait(barrier, greeted)
        for side in range(2):
            when_do(straight(side), lambda: edge_copy(side, c).start())
        for side in range(2):
            if detour:
                when_do(middle(side), lambda: edge_copy(side, c).start())
            when_do(target("gy", side), lambda: y_bulk_copy(side, c).start())
        if c in relayed:
            send_inner(c)
        if 0 <= at - BEHIND < EARLY_BULK:
            send_outer(order[at - BEHIND])
    for c in order[min(EARLY_BULK, max(count - BEHIND, 0)) :]:
        send_outer(c)
    for c in order:
        if c not in relayed:
            send_inner(c)
    while waiting or edging:
        if edging:
            y_edges(edging.pop(0))
        if waiting and count - len(edging) >= EDGES_FIRST:
            forward(waiting.pop(0))

    def xy_sum(comp, n, lanes):
        value = local[comp, n, :, lanes]
        rows = []
        for side in range(2):
            tile, row = y_seat(side, comp, n)
            rows.append(y_in[side, tile, row : row + 1, lanes])
        if n in (0, 7):
            side = 0 if n == 0 else 1
            tiles = [x_in[side, tile, :, lanes] for tile in range(comps)]
            value = value + unpack(tiles, comp, X_EDGE)
        where = row_index(value.shape)
        return value + jnp.where(where == 0, rows[0], jnp.where(where == 7, rows[1], 0.0))

    def arrived(c):
        landed("gx", x_in.at[:, 1:, :, span_of(c)], bulk_recv.at[c])
        landed("gy", y_in.at[:, 0, :, span_of(c)], y_recv.at[c])

    every = [(comp, n) for comp in range(comps) for n in range(8)]
    inner = [
        (comp, n)
        for comp, n in every
        if n not in (0, 7) and y_seat(0, comp, n)[0] and y_seat(1, comp, n)[0]
    ]
    outside = [which for which in every if which not in inner]

    def finish(first, last, planes=every):
        for comp, n in planes:
            value = xy_sum(comp, n, slice(max(first - LANES, 0), min(last + LANES, total)))
            if first == 0:
                value = jnp.concatenate([z_in[0, comp, n], value], axis=1)
            if last == total:
                value = jnp.concatenate([value, z_in[1, comp, n]], axis=1)
            width = value.shape[1]
            before = pltpu.roll(value, 1, 1)[:, LANES:-LANES]
            after = pltpu.roll(value, width - 1, 1)[:, LANES:-LANES]
            position = lax.broadcasted_iota(jnp.int32, before.shape, 1) % 8
            extra = jnp.where(position == 7, after, jnp.where(position == 0, before, 0.0))
            out[comp, n, :, first:last] = value[:, LANES:-LANES] + extra

    def sent(name, ref, send):
        def wait(part):
            remote(part, part, send, send, beside(name, 0)).wait_send()

        if sizes[name] == 2:
            wait(ref.at[0])
        elif sizes[name] > 2:
            both = jnp.logical_and(below[name], above[name])
            when_do(both, lambda: wait(ref))
            when_do(jnp.logical_not(both), lambda: wait(ref.at[0]))

    def onward_sent():
        part = relay.at[:, :, pl.ds(0, sum(spans[c][1] for c in relayed))]
        remote(part, part, r_send.at[0], r_send.at[0], beside("gz", 0)).wait_send()

    def finish_outer():
        when_do(above["gz"], lambda: z_copy(1).wait_recv())
        finish(total - LANES, total)
        when_do(jnp.logical_not(below["gz"]), lambda: finish(0, LANES))

    def finish_first():
        z_copy(0).wait_recv()
        finish(0, LANES)

    tiles = total // LANES
    outer = {0, tiles - 1}
    todo, here = set(range(tiles)) - outer, set()
    ends_here = False
    landed("gy", y_in.at[:, 1:], y_bulk_recv.at[0])
    for first in range(LANES, total - LANES, INNER):
        finish(first, min(first + INNER, total - LANES), inner)
    for at, c in enumerate(order):
        if at == count - 1 - OUTER_EARLY and at >= 2:
            finish_outer()
        arrived(c)
        here |= set(range(spans[c][0] // LANES, sum(spans[c]) // LANES))
        if outer <= here and not ends_here:
            ends_here = True
            for side in range(2):
                lanes = slice(total - LANES, total) if side == 0 else slice(0, LANES)
                for comp in range(comps):
                    for n in range(8):
                        z_out[side, comp, n] = xy_sum(comp, n, lanes)
                when_do(target("gz", side), lambda: z_copy(side).start())
        ready = sorted(t for t in todo if {t - 1, t, t + 1} <= here)
        todo -= set(ready)
        while ready:
            first = last = ready.pop(0)
            while ready and ready[0] == last + 1:
                last = ready.pop(0)
            finish(first * LANES, (last + 1) * LANES, outside)
    if count - 1 - OUTER_EARLY not in range(2, count):
        finish_outer()

    when_do(below["gz"], finish_first)

    sent("gx", x_out, x_send.at[0])
    sent("gy", y_out, y_send.at[0])
    sent("gz", z_out, z_send.at[0])
    if relayed:
        when_do(jnp.logical_or(place["gx"] == 0, place["gx"] == 3), onward_sent)


def local_part(sizes, nodal_scalar_values, geometry):
    comps, _, _, total = nodal_scalar_values.shape
    spans = chunk_spans(total)
    count = len(spans)
    matrices, scales = tables()
    f32 = jnp.float32
    dma = pltpu.SemaphoreType.DMA
    any_space = pl.BlockSpec(memory_space=pl.ANY)
    plane = pltpu.VMEM((2, comps, 8, total), f32)
    column = pltpu.VMEM((2, comps, 8, 8, LANES), f32)
    return pl.pallas_call(
        functools.partial(kernel, sizes, spans),
        out_shape=pltpu.VMEM(nodal_scalar_values.shape, f32),
        in_specs=[any_space] * 4,
        out_specs=pl.BlockSpec(memory_space=pltpu.VMEM),
        scratch_shapes=[
            pltpu.VMEM(nodal_scalar_values.shape, f32),
            pltpu.VMEM(geometry.shape, f32),
            pltpu.VMEM(matrices.shape, jnp.bfloat16),
            pltpu.VMEM(scales.shape, f32),
            pltpu.VMEM((8, total), f32),
            pltpu.VMEM(nodal_scalar_values.shape, f32),
            plane,
            plane,
            plane,
            plane,
            column,
            column,
            pltpu.VMEM((comps - 1, 8, total), f32),
            dma((min(count, 3),)),
            dma((3,)),
            dma((1,)),
            dma((1,)),
            dma((1,)),
            dma((1,)),
            dma((count,)),
            dma((count,)),
            dma((count,)),
            dma((1,)),
            dma((2,)),
            dma((max(len(relayed_chunks(spans)), 1),)),
        ],
        compiler_params=pltpu.CompilerParams(collective_id=0, has_side_effects=True),
        name="poisson",
    )(nodal_scalar_values, geometry, jnp.asarray(matrices), jnp.asarray(scales))


def solution(mesh):
    return jax.shard_map(
        functools.partial(local_part, dict(mesh.shape)),
        mesh=mesh,
        in_specs=(P(None, "gx", "gy", "gz"), P(None, "gx", "gy", "gz")),
        out_specs=P(None, "gx", "gy", "gz"),
        check_vma=False,
    )
```

```python
import functools

import jax
import jax.numpy as jnp
import numpy as np
from jax import lax
from jax.experimental import pallas as pl
from jax.experimental.pallas import tpu as pltpu
from jax.sharding import PartitionSpec as P

interior_points = [
    -0.8717401485096066,
    -0.5917001814331423,
    -0.2092992179024789,
    0.2092992179024789,
    0.5917001814331423,
    0.8717401485096066,
]
MESH = pl.DeviceIdType.MESH
STEP = 512
LANES = 128
X_FIRST = True
BEHIND = 1
EARLY_BULK = 2
RELAYED = 3
EDGES_FIRST = 2
OUTER_EARLY = 0
INNER = 256
X_EDGE = 7
Y_EDGE = (6, 7)


def legendre_seven(point):
    previous = 1.0
    current = point
    for order in range(1, 7):
        following = ((2 * order + 1) * point * current - order * previous) / (order + 1)
        previous = current
        current = following
    return current


def gll_tables():
    degree = 7
    points = [-1.0] + interior_points + [1.0]
    values = [legendre_seven(point) for point in points]
    node_count = degree + 1
    weights = np.array([2.0 / (degree * (degree + 1) * value * value) for value in values])
    derivative = np.zeros((node_count, node_count))
    for row_index in range(node_count):
        for col_index in range(node_count):
            if row_index != col_index:
                derivative[row_index, col_index] = values[row_index] / (
                    values[col_index] * (points[row_index] - points[col_index])
                )
    derivative[0, 0] = -degree * (degree + 1) / 4.0
    derivative[node_count - 1, node_count - 1] = degree * (degree + 1) / 4.0
    return (derivative, weights)


def halves(table):
    table = np.asarray(table, np.float32)
    high = table.astype(jnp.bfloat16)
    low = (table - high.astype(np.float32)).astype(jnp.bfloat16)
    return high, low


def tables():
    derivative, weights = gll_tables()
    eye = np.eye(8)
    plane_weight = np.kron(weights, weights)
    forward_xy = np.concatenate([np.kron(derivative, eye), np.kron(eye, derivative)], axis=0)
    back_xy = np.concatenate([np.kron(derivative.T, eye), np.kron(eye, derivative.T)], axis=1)
    back_xy = back_xy * np.tile(plane_weight, 2)[None, :]
    forward_z = np.kron(np.eye(16), derivative.T)
    back_z = np.kron(np.eye(16), derivative)
    high, low = halves(forward_xy)
    forward_xy = np.concatenate([high, high, low, low], axis=1)
    high, low = halves(back_xy)
    back_xy = np.concatenate(
        [np.concatenate([high, high], axis=1), np.concatenate([low, low], axis=1)], axis=0
    )
    high, low = halves(forward_z)
    forward_z = np.tile(np.concatenate([high, low], axis=1), (2, 1))
    high, low = halves(back_z)
    back_z = np.tile(np.concatenate([high, low], axis=1), (2, 1))
    matrices = np.concatenate([forward_xy, back_xy, forward_z, back_z], axis=0)
    plane = np.repeat(plane_weight[:, None], LANES, axis=1)
    along = np.repeat(np.tile(weights, LANES // 8)[None, :], 8, axis=0)
    scales = np.concatenate([plane, along], axis=0).astype(np.float32)
    return matrices, scales


def row_index(shape):
    return lax.broadcasted_iota(jnp.int32, shape, 0)


def pack(planes, edge):
    first, second, third = planes
    turn = (row_index(first.shape) + (8 - edge)) % 8
    own = turn < 2
    second_edge = jnp.logical_and(turn >= 2, turn < 4)
    third_edge = jnp.logical_and(turn >= 4, turn < 6)
    edges = jnp.where(
        second_edge,
        pltpu.roll(second, 2, 0),
        jnp.where(third_edge, pltpu.roll(third, 4, 0), first),
    )
    return [
        edges,
        jnp.where(own, pltpu.roll(first, 6, 0), second),
        jnp.where(own, pltpu.roll(first, 4, 0), third),
    ]


def unpack(tiles, comp, edge):
    turn = (row_index(tiles[0].shape) + (8 - edge)) % 8
    if comp:
        return jnp.where(turn < 2, pltpu.roll(tiles[0], 8 - 2 * comp, 0), tiles[comp])
    from_second = jnp.logical_and(turn >= 2, turn < 4)
    from_third = jnp.logical_and(turn >= 4, turn < 6)
    return jnp.where(
        from_second,
        pltpu.roll(tiles[1], 2, 0),
        jnp.where(from_third, pltpu.roll(tiles[2], 4, 0), tiles[0]),
    )


def y_planes(terms):
    turn = (row_index(terms[0].shape) + 1) % 8

    def gather(four):
        return jnp.where(
            turn < 2,
            four[0],
            jnp.where(
                turn < 4,
                pltpu.roll(four[1], 2, 0),
                jnp.where(turn < 6, pltpu.roll(four[2], 4, 0), pltpu.roll(four[3], 6, 0)),
            ),
        )

    low, high = gather(terms[:4]), pltpu.roll(gather(terms[4:]), 1, 0)
    even = turn % 2 == 0
    return jnp.where(even, low, high), jnp.where(even, high, low)


def y_seat(side, comp, n):
    edge = Y_EDGE[side]
    row = (2 * n + 7 + side) % 8 if n < 4 else 2 * (n - 4) + side
    turn = (row - edge) % 8
    if turn < 2:
        return 0, (row + 2 * comp) % 8
    if comp:
        return comp, row
    if turn < 6:
        return turn // 2, (row - 2 * (turn // 2)) % 8
    return 0, row


def split(value):
    high = value.astype(jnp.bfloat16)
    low = (value - high.astype(jnp.float32)).astype(jnp.bfloat16)
    return high, low


def product(left, right):
    return jnp.dot(left, right, preferred_element_type=jnp.float32)


def along_lanes(pairs, table):
    rows, width = pairs[0][0].shape
    spans = [slice(start, start + LANES) for start in range(0, width, LANES)]
    stacked = [
        jnp.concatenate([high[:, span], low[:, span]], axis=1)
        for high, low in pairs
        for span in spans
    ]
    twice = product(jnp.concatenate(stacked, axis=0), table)
    once = twice[:, :LANES] + twice[:, LANES:]
    pieces = [once[at * rows : (at + 1) * rows] for at in range(len(stacked))]
    return [
        jnp.concatenate(pieces[at : at + len(spans)], axis=1)
        for at in range(0, len(pieces), len(spans))
    ]


def chunk_spans(total):
    if total % STEP or total < 2 * STEP:
        return [(0, total)]
    widths = [STEP // 2] + [STEP] * (total // STEP - 1) + [STEP // 2]
    starts = [sum(widths[:at]) for at in range(len(widths))]
    return list(zip(starts, widths))


def chunk_order(count):
    return [0] + ([count - 1] if count > 1 else []) + list(range(1, count - 1))


def relayed_chunks(spans):
    total = sum(width for _, width in spans)
    chosen, lanes = [], 0
    for c in chunk_order(len(spans)):
        if (lanes + spans[c][1]) * 4 <= total * RELAYED:
            chosen.append(c)
            lanes += spans[c][1]
    return chosen


def kernel(
    sizes,
    spans,
    u_hbm,
    geo_hbm,
    mat_hbm,
    scale_hbm,
    out,
    u,
    geo,
    mat,
    scale,
    metric,
    local,
    x_out,
    y_out,
    x_in,
    y_in,
    z_out,
    z_in,
    relay,
    in_sem,
    const_sem,
    edge_recv,
    bulk_recv,
    y_recv,
    y_bulk_recv,
    z_recv,
    r_recv,
):
    comps, _, _, total = u.shape
    count = len(spans)
    order = chunk_order(count)
    names = ("gx", "gy", "gz")
    place = {name: lax.axis_index(name) for name in names}
    below = {name: place[name] > 0 for name in names}
    above = {name: place[name] < sizes[name] - 1 for name in names}

    const_copies = [
        pltpu.make_async_copy(mat_hbm, mat, const_sem.at[0]),
        pltpu.make_async_copy(scale_hbm, scale, const_sem.at[1]),
        pltpu.make_async_copy(geo_hbm, geo, const_sem.at[2]),
    ]
    for copy in const_copies:
        copy.start()
    in_copies = {}
    loads = [[c] for c in order[:2]] + ([sorted(order[2:])] if count > 2 else [])
    for at, members in enumerate(loads):
        span = pl.ds(spans[members[0]][0], sum(spans[c][1] for c in members))
        in_copies[members[0]] = pltpu.make_async_copy(
            u_hbm.at[:, :, :, span], u.at[:, :, :, span], in_sem.at[at]
        )
        in_copies[members[0]].start()

    barrier = pltpu.get_barrier_semaphore()
    for name in names:
        for there, by in ((below[name], -1), (above[name], 1)):

            @pl.when(there)
            def _(name=name, by=by):
                pl.semaphore_signal(
                    barrier, inc=1, device_id={name: place[name] + by}, device_id_type=MESH
                )

    detour = sizes["gx"] == 4
    relayed = relayed_chunks(spans) if detour else []
    opposite = lax.rem(place["gx"] + 2, 4)
    if detour:
        pl.semaphore_signal(barrier, inc=1, device_id={"gx": opposite}, device_id_type=MESH)

    for side in range(2):
        there = below if side == 0 else above

        @pl.when(jnp.logical_not(there["gx"]))
        def _(side=side):
            x_in[side] = jnp.zeros(x_in.shape[1:], jnp.float32)

        @pl.when(jnp.logical_not(there["gy"]))
        def _(side=side):
            y_in[side] = jnp.zeros(y_in.shape[1:], jnp.float32)

        @pl.when(jnp.logical_not(there["gz"]))
        def _(side=side):
            z_in[side] = jnp.zeros(z_in.shape[1:], jnp.float32)

    for copy in const_copies:
        copy.wait()

    rows = jnp.concatenate(
        [geo[k, 0] for k in range(6)] + [jnp.zeros((2, geo.shape[-1]), jnp.float32)], axis=0
    )
    lane = lax.broadcasted_iota(jnp.int32, (8, LANES), 1)
    for tile in range(total // LANES):
        first = tile * (LANES // 8)
        block = rows[:, first // LANES * LANES : first // LANES * LANES + LANES]
        spread = jnp.take_along_axis(block, lane // 8 + first % LANES, axis=1)
        metric[:, tile * LANES : (tile + 1) * LANES] = spread * scale[64:72, :]

    def span_of(c):
        return pl.ds(*spans[c])

    def beside(name, side):
        return {name: place[name] + (1 if side == 0 else -1)}

    def remote(source, target, send, recv, device):
        return pltpu.make_async_remote_copy(
            source, target, send, recv, device_id=device, device_id_type=MESH
        )

    def edge_copy(side, c):
        at = (side, 0, slice(None), span_of(c))
        return remote(
            x_out.at[at], x_in.at[at], const_sem.at[0], edge_recv.at[c], beside("gx", side)
        )

    def bulk_copy(side, c):
        at = (side, slice(1, None), slice(None), span_of(c))
        return remote(
            x_out.at[at],
            x_in.at[at],
            const_sem.at[0],
            bulk_recv.at[c],
            beside("gx", side),
        )

    def y_edge_copy(side, c):
        at = (side, 0, slice(None), span_of(c))
        return remote(
            y_out.at[at], y_in.at[at], const_sem.at[1], y_recv.at[c], beside("gy", side)
        )

    def y_bulk_copy(side, c):
        at = (side, slice(1, None), slice(None), span_of(c))
        return remote(
            y_out.at[at], y_in.at[at], const_sem.at[1], y_bulk_recv.at[0], beside("gy", side)
        )

    def z_copy(side):
        return remote(
            z_out.at[side], z_in.at[side], const_sem.at[2], z_recv.at[side], beside("gz", side)
        )

    def middle(side):
        return place["gx"] == 1 + side

    def by_way_of(side):
        return 3 * (1 - side) if X_FIRST else 3 * side

    def hop_copy(side, c):
        return remote(
            x_out.at[side, 1:, :, span_of(c)],
            relay.at[:, :, span_of(c)],
            const_sem.at[0],
            r_recv.at[relayed.index(c)],
            {"gx": by_way_of(side)},
        )

    def onward_copy(side, c):
        return remote(
            relay.at[:, :, span_of(c)],
            x_in.at[side, 1:, :, span_of(c)],
            in_sem.at[0],
            bulk_recv.at[c],
            {"gx": 2 - side},
        )

    def target(name, side):
        return above[name] if side == 0 else below[name]

    def source(name, side):
        return below[name] if side == 0 else above[name]

    def when_do(condition, act):
        @pl.when(condition)
        def _():
            act()

    def landed(name, ref, recv):
        def wait(part):
            remote(part, part, recv, recv, beside(name, 0)).wait_recv()

        if sizes[name] == 2:
            wait(ref.at[0])
        elif sizes[name] > 2:
            both = jnp.logical_and(below[name], above[name])
            when_do(both, lambda: wait(ref))
            when_do(jnp.logical_not(both), lambda: wait(ref.at[0]))

    def forward(c):
        for side in range(2):

            @pl.when(place["gx"] == by_way_of(side))
            def _(side=side):
                hop_copy(side, c).wait_recv()
                onward_copy(side, c).start()

    def straight(side):
        if detour:
            return jnp.logical_and(target("gx", side), jnp.logical_not(middle(side)))
        return target("gx", side)

    def send_outer(c):
        for side in range(2):
            when_do(straight(side), lambda: bulk_copy(side, c).start())

    def send_inner(c):
        for side in range(2):
            if c in relayed:
                when_do(middle(side), lambda: hop_copy(side, c).start())
            elif detour:
                when_do(middle(side), lambda: bulk_copy(side, c).start())

    def y_edges(c):
        lanes = slice(spans[c][0], sum(spans[c]))
        landed("gx", x_in.at[:, 0, :, span_of(c)], edge_recv.at[c])
        low, high = x_in[0, 0, :, lanes], pltpu.roll(x_in[1, 0, :, lanes], 7, 0)
        for side in range(2):
            turn = (row_index(low.shape) + (8 - Y_EDGE[side])) % 8
            extra = jnp.where(turn % 2 == 1, low, high)
            extra = jnp.where(turn < 6, extra, 0.0)
            y_out[side, 0, :, lanes] = y_out[side, 0, :, lanes] + extra
        for side in range(2):
            when_do(target("gy", side), lambda: y_edge_copy(side, c).start())

    forward_xy, back_xy = mat[0:128, :], mat[128:256, :]
    forward_z, back_z = mat[256:512, :], mat[512:768, :]

    greeted = sum(side[name].astype(jnp.int32) for name in names for side in (below, above))
    greeted = greeted + (1 if detour else 0)
    waiting, edging = list(relayed), list(order)
    for at, c in enumerate(order):
        if c in in_copies:
            in_copies[c].wait()
        step = spans[c][1]
        for start in (spans[c][0],):
            lanes = slice(start, start + step)
            g00, g11, g22, g01, g02, g12 = [metric[k : k + 1, lanes] for k in range(6)]
            pairs = [split(u[comp, :, :, lanes].reshape(64, step)) for comp in range(comps)]
            planes = [
                product(forward_xy, jnp.concatenate([high, low, high, low], axis=0))
                for high, low in pairs
            ]
            grads_z = along_lanes(pairs, forward_z)
            sums, z_pairs = [], []
            for both, grad_z in zip(planes, grads_z):
                grad_x, grad_y = both[:64], both[64:]
                flux_x = g00 * grad_x + g01 * grad_y + g02 * grad_z
                flux_y = g01 * grad_x + g11 * grad_y + g12 * grad_z
                x_high, x_low = split(flux_x)
                y_high, y_low = split(flux_y)
                z_pairs.append(split(g02 * grad_x + g12 * grad_y + g22 * grad_z))
                sums.append(
                    product(back_xy, jnp.concatenate([x_high, y_high, x_low, y_low], axis=0))
                )
            backs_z = along_lanes(z_pairs, back_z)
            weight = jnp.concatenate([scale[0:64, :]] * (step // LANES), axis=1)
            ends = ([], [])
            sides = ([], [])
            for comp in range(comps):
                twice = sums[comp]
                terms = twice[:64] + twice[64:] + weight * backs_z[comp]
                terms = terms.reshape(8, 8, step)
                local[comp, :, :, lanes] = terms
                for side, plane in enumerate(y_planes([terms[n] for n in range(8)])):
                    sides[side].append(plane)
                    ends[side].append(terms[7 if side == 0 else 0])
            for side in range(2):
                for tile, value in enumerate(pack(ends[side], X_EDGE)):
                    x_out[side, tile, :, lanes] = value
                for tile, value in enumerate(pack(sides[side], Y_EDGE[side])):
                    y_out[side, tile, :, lanes] = value
        if at == 0:
            pl.semaphore_wait(barrier, greeted)
        for side in range(2):
            when_do(straight(side), lambda: edge_copy(side, c).start())
        for side in range(2):
            if detour:

                @pl.when(middle(side))
                def _(side=side):
                    edge_copy(side, c).start()
                    if c in relayed:
                        hop_copy(side, c).start()

            when_do(target("gy", side), lambda: y_bulk_copy(side, c).start())
        if 0 <= at - BEHIND < EARLY_BULK:
            send_outer(order[at - BEHIND])
    for c in order[min(EARLY_BULK, max(count - BEHIND, 0)) :]:
        send_outer(c)
    for c in order:
        if c not in relayed:
            send_inner(c)
    while waiting or edging:
        if edging:
            y_edges(edging.pop(0))
        if waiting and count - len(edging) >= EDGES_FIRST:
            forward(waiting.pop(0))

    def xy_sum(comp, n, lanes):
        value = local[comp, n, :, lanes]
        rows = []
        for side in range(2):
            tile, row = y_seat(side, comp, n)
            rows.append(y_in[side, tile, row : row + 1, lanes])
        if n in (0, 7):
            side = 0 if n == 0 else 1
            tiles = [x_in[side, tile, :, lanes] for tile in range(comps)]
            value = value + unpack(tiles, comp, X_EDGE)
        where = row_index(value.shape)
        return value + jnp.where(where == 0, rows[0], jnp.where(where == 7, rows[1], 0.0))

    def arrived(c):
        landed("gx", x_in.at[:, 1:, :, span_of(c)], bulk_recv.at[c])
        landed("gy", y_in.at[:, 0, :, span_of(c)], y_recv.at[c])

    every = [(comp, n) for comp in range(comps) for n in range(8)]
    inner = [
        (comp, n)
        for comp, n in every
        if n not in (0, 7) and y_seat(0, comp, n)[0] and y_seat(1, comp, n)[0]
    ]
    outside = [which for which in every if which not in inner]

    def finish(first, last, planes=every):
        for comp, n in planes:
            value = xy_sum(comp, n, slice(max(first - LANES, 0), min(last + LANES, total)))
            if first == 0:
                value = jnp.concatenate([z_in[0, comp, n], value], axis=1)
            if last == total:
                value = jnp.concatenate([value, z_in[1, comp, n]], axis=1)
            width = value.shape[1]
            before = pltpu.roll(value, 1, 1)[:, LANES:-LANES]
            after = pltpu.roll(value, width - 1, 1)[:, LANES:-LANES]
            position = lax.broadcasted_iota(jnp.int32, before.shape, 1) % 8
            extra = jnp.where(position == 7, after, jnp.where(position == 0, before, 0.0))
            out[comp, n, :, first:last] = value[:, LANES:-LANES] + extra

    def sent(name, ref, send):
        def wait(part):
            remote(part, part, send, send, beside(name, 0)).wait_send()

        if sizes[name] == 2:
            wait(ref.at[0])
        elif sizes[name] > 2:
            both = jnp.logical_and(below[name], above[name])
            when_do(both, lambda: wait(ref))
            when_do(jnp.logical_not(both), lambda: wait(ref.at[0]))

    def onward_sent():
        part = relay.at[:, :, pl.ds(0, sum(spans[c][1] for c in relayed))]
        remote(part, part, in_sem.at[0], in_sem.at[0], beside("gz", 0)).wait_send()

    def finish_outer():
        when_do(above["gz"], lambda: z_copy(1).wait_recv())
        finish(total - LANES, total)
        when_do(jnp.logical_not(below["gz"]), lambda: finish(0, LANES))

    def finish_first():
        z_copy(0).wait_recv()
        finish(0, LANES)

    tiles = total // LANES
    outer = {0, tiles - 1}
    todo, here = set(range(tiles)) - outer, set()
    ends_here = False
    landed("gy", y_in.at[:, 1:], y_bulk_recv.at[0])
    for first in range(LANES, total - LANES, INNER):
        finish(first, min(first + INNER, total - LANES), inner)
    for at, c in enumerate(order):
        if at == count - 1 - OUTER_EARLY and at >= 2:
            finish_outer()
        arrived(c)
        here |= set(range(spans[c][0] // LANES, sum(spans[c]) // LANES))
        if outer <= here and not ends_here:
            ends_here = True
            for side in range(2):
                lanes = slice(total - LANES, total) if side == 0 else slice(0, LANES)
                for comp in range(comps):
                    for n in range(8):
                        z_out[side, comp, n] = xy_sum(comp, n, lanes)
                when_do(target("gz", side), lambda: z_copy(side).start())
        ready = sorted(t for t in todo if {t - 1, t, t + 1} <= here)
        todo -= set(ready)
        while ready:
            first = last = ready.pop(0)
            while ready and ready[0] == last + 1:
                last = ready.pop(0)
            finish(first * LANES, (last + 1) * LANES, outside)
    if count - 1 - OUTER_EARLY not in range(2, count):
        finish_outer()

    when_do(below["gz"], finish_first)

    sent("gx", x_out, const_sem.at[0])
    sent("gy", y_out, const_sem.at[1])
    sent("gz", z_out, const_sem.at[2])
    if relayed:
        when_do(jnp.logical_or(place["gx"] == 0, place["gx"] == 3), onward_sent)


def local_part(sizes, nodal_scalar_values, geometry):
    comps, _, _, total = nodal_scalar_values.shape
    spans = chunk_spans(total)
    count = len(spans)
    matrices, scales = tables()
    f32 = jnp.float32
    dma = pltpu.SemaphoreType.DMA
    any_space = pl.BlockSpec(memory_space=pl.ANY)
    plane = pltpu.VMEM((2, comps, 8, total), f32)
    column = pltpu.VMEM((2, comps, 8, 8, LANES), f32)
    return pl.pallas_call(
        functools.partial(kernel, sizes, spans),
        out_shape=pltpu.VMEM(nodal_scalar_values.shape, f32),
        in_specs=[any_space] * 4,
        out_specs=pl.BlockSpec(memory_space=pltpu.VMEM),
        scratch_shapes=[
            pltpu.VMEM(nodal_scalar_values.shape, f32),
            pltpu.VMEM(geometry.shape, f32),
            pltpu.VMEM(matrices.shape, jnp.bfloat16),
            pltpu.VMEM(scales.shape, f32),
            pltpu.VMEM((8, total), f32),
            pltpu.VMEM(nodal_scalar_values.shape, f32),
            plane,
            plane,
            plane,
            plane,
            column,
            column,
            pltpu.VMEM((comps - 1, 8, total), f32),
            dma((min(count, 3),)),
            dma((3,)),
            dma((count,)),
            dma((count,)),
            dma((count,)),
            dma((1,)),
            dma((2,)),
            dma((max(len(relayed_chunks(spans)), 1),)),
        ],
        compiler_params=pltpu.CompilerParams(collective_id=0, has_side_effects=True),
        name="poisson",
    )(nodal_scalar_values, geometry, jnp.asarray(matrices), jnp.asarray(scales))


def solution(mesh):
    return jax.shard_map(
        functools.partial(local_part, dict(mesh.shape)),
        mesh=mesh,
        in_specs=(P(None, "gx", "gy", "gz"), P(None, "gx", "gy", "gz")),
        out_specs=P(None, "gx", "gy", "gz"),
        check_vma=False,
    )
```
